64 devices in a mesh: dp: 4 (over x, y), tp: 16 (over z, core).
Axes of the slice: x: 2, y: 2, z: 8, core: 2. Of those that a mesh axis runs over, the one named last changes fastest.
The devices are a block of a 4x4x8 slice.
Arguments:
- token_ids: int32 [32768], P('dp'), parts along dimension 0
- emb_table: bfloat16 [32128, 512], P('tp')
- norm_gain: bfloat16 [512], replicated
- w_in: bfloat16 [512, 2048], P(None, 'tp')
- w_out: bfloat16 [2048, 512], P('tp')
- d_out: bfloat16 [32768, 512], P(('dp', 'tp')), parts along dimension 0
Outputs:
- output 1: bfloat16 [32768, 512], P(('dp', 'tp')), parts along dimension 0
- output 2: float32 [128512, 512], P(('dp', 'tp')), parts along dimension 0
- output 3: float32 [2048, 2048], P('dp', 'tp'), parts along dimension 0
- output 4: float32 [8192, 512], P(('dp', 'tp')), parts along dimension 0
There are 4 independent parts. The reference program is written for one: setup_inputs(seed, part) draws one part's arguments, and reference() takes and returns one part's arrays. A program takes and returns all parts, laid end to end along the dimension named above; an argument that names none is the same for every part.
All inputs are finite; a program needn't handle non-finite values.
Results may differ from the reference program's by a relative error of at most 0.00935178.
Values are sent between devices in bfloat16 or wider.
A program may use at most 768 MiB of HBM per device.

```python
import math
import jax
import jax.numpy as jnp
from jax import lax

VOCAB_SIZE = 32128
MODEL_DIM = 512
HIDDEN_DIM = 2048
TOKENS = 8192

EPS = 1e-6
VOCAB_BITS = math.ceil(math.log2(VOCAB_SIZE))


def draw_ids(id_key):
    key_level, key_zipf, key_flat, key_pick = jax.random.split(id_key, 4)
    bit_level = jax.random.randint(key_level, (TOKENS,), 0, VOCAB_BITS + 1, dtype=jnp.int32)
    id_span = jnp.left_shift(jnp.ones_like(bit_level), bit_level)
    zipf_ids = jax.random.randint(key_zipf, (TOKENS,), 0, id_span, dtype=jnp.int32) % VOCAB_SIZE
    flat_ids = jax.random.randint(key_flat, (TOKENS,), 0, VOCAB_SIZE, dtype=jnp.int32)
    choice = jax.random.randint(key_pick, (TOKENS,), 0, 10, dtype=jnp.int32)
    mixed_ids = jnp.where(choice < 7, zipf_ids, flat_ids)
    end_ids = jnp.array([0, VOCAB_SIZE - 1], dtype=jnp.int32)
    return jnp.concatenate([end_ids, mixed_ids[2:]]).astype(jnp.int32)


def setup_inputs(seed: int = 0, part: int = 0) -> dict:
    key_table, key_gain, key_in, key_out = jax.random.split(jax.random.key(seed), 4)
    part_key = jax.random.fold_in(jax.random.key(seed + 1), part)
    key_ids, key_dout = jax.random.split(part_key, 2)
    emb_table = jax.random.normal(key_table, (VOCAB_SIZE, MODEL_DIM), jnp.float32).astype(jnp.bfloat16)
    norm_gain = (1.0 + 0.5 * jax.random.normal(key_gain, (MODEL_DIM,), jnp.float32)).astype(jnp.bfloat16)
    w_in = (jax.random.normal(key_in, (MODEL_DIM, HIDDEN_DIM), jnp.float32) * MODEL_DIM ** -0.5).astype(jnp.bfloat16)
    w_out = (jax.random.normal(key_out, (HIDDEN_DIM, MODEL_DIM), jnp.float32) * (1.5 * HIDDEN_DIM ** -0.5)).astype(jnp.bfloat16)
    token_ids = draw_ids(key_ids)
    d_out = (jax.random.normal(key_dout, (TOKENS, MODEL_DIM), jnp.float32) * TOKENS ** -0.5).astype(jnp.bfloat16)
    return {"token_ids": token_ids, "emb_table": emb_table, "norm_gain": norm_gain, "w_in": w_in, "w_out": w_out, "d_out": d_out}


def reference(token_ids, emb_table, norm_gain, w_in, w_out, d_out):
    embedded = jnp.take(emb_table, token_ids, axis=0)
    embedded_f32 = embedded.astype(jnp.float32)
    inv_rms = lax.rsqrt(jnp.mean(embedded_f32 * embedded_f32, axis=-1, keepdims=True) + EPS)
    gain_f32 = norm_gain.astype(jnp.float32)
    normed = (embedded_f32 * inv_rms * gain_f32).astype(jnp.bfloat16)
    pre_act = jnp.dot(normed, w_in, preferred_element_type=jnp.float32).astype(jnp.bfloat16)
    act_f32, gelu_vjp = jax.vjp(jax.nn.gelu, pre_act.astype(jnp.float32))
    hidden = act_f32.astype(jnp.bfloat16)
    mlp_out = jnp.dot(hidden, w_out, preferred_element_type=jnp.float32)
    block_out = (embedded_f32 + mlp_out).astype(jnp.bfloat16)
    d_hidden = jnp.dot(d_out, w_out.T, preferred_element_type=jnp.float32).astype(jnp.bfloat16)
    d_w_out = jnp.dot(hidden.T, d_out, preferred_element_type=jnp.float32)
    (d_pre_f32,) = gelu_vjp(d_hidden.astype(jnp.float32))
    d_pre = d_pre_f32.astype(jnp.bfloat16)
    d_w_in = jnp.dot(normed.T, d_pre, preferred_element_type=jnp.float32)
    d_normed = jnp.dot(d_pre, w_in.T, preferred_element_type=jnp.float32)
    d_scaled = d_normed * gain_f32
    row_proj = jnp.mean(d_scaled * embedded_f32, axis=-1, keepdims=True)
    d_emb = (d_out.astype(jnp.float32) + inv_rms * (d_scaled - embedded_f32 * inv_rms * inv_rms * row_proj)).astype(jnp.bfloat16)
    d_table = jax.ops.segment_sum(d_emb.astype(jnp.float32), token_ids, num_segments=VOCAB_SIZE)
    return block_out, d_table, d_w_in, d_w_out
```

```python
import jax
import jax.numpy as jnp
from jax import lax
from jax.sharding import PartitionSpec as P

EPS = 1e-6


def solution(mesh):
    tp = mesh.shape["tp"]

    def shard_step(token_ids, emb_table, norm_gain, w_in, w_out, d_out):
        f32, bf16 = jnp.float32, jnp.bfloat16
        rank = lax.axis_index("tp")
        vocab_local, dim = emb_table.shape
        hid = w_out.shape[0]
        local_ids = token_ids - rank * vocab_local
        weights = lax.all_gather(jnp.concatenate([w_in.T, w_out], axis=0), "tp", axis=0, tiled=False)
        w_in_t = weights[:, :hid].reshape(tp * hid, dim)
        w_out_full = weights[:, hid:].reshape(tp * hid, dim)
        pick = (local_ids[:, None] == lax.broadcasted_iota(jnp.int32, (token_ids.shape[0], vocab_local), 1)).astype(bf16)
        lookup_part = jnp.dot(pick, emb_table, preferred_element_type=f32).astype(bf16)
        embedded = lax.psum_scatter(lookup_part, "tp", scatter_dimension=0, tiled=True)
        x = embedded.astype(f32)
        inv_rms = lax.rsqrt(jnp.mean(x * x, axis=-1, keepdims=True) + EPS)
        gain = norm_gain.astype(f32)
        normed = (x * inv_rms * gain).astype(bf16)
        pre_act = lax.dot_general(normed, w_in_t, (((1,), (1,)), ((), ())), preferred_element_type=f32).astype(bf16)
        act, gelu_vjp = jax.vjp(jax.nn.gelu, pre_act.astype(f32))
        hidden = act.astype(bf16)
        y = jnp.dot(hidden, w_out_full, preferred_element_type=f32)
        block_out = (x + y).astype(bf16)

        d_hidden = lax.dot_general(d_out, w_out_full, (((1,), (1,)), ((), ())), preferred_element_type=f32).astype(bf16)
        (d_pre_f32,) = gelu_vjp(d_hidden.astype(f32))
        d_pre = d_pre_f32.astype(bf16)
        d_normed = jnp.dot(d_pre, w_in_t, preferred_element_type=f32)
        d_scaled = d_normed * gain
        row_proj = jnp.mean(d_scaled * x, axis=-1, keepdims=True)
        d_emb = (d_out.astype(f32) + inv_rms * (d_scaled - x * inv_rms * inv_rms * row_proj)).astype(bf16)
        d_emb_full = lax.all_gather(d_emb, "tp", axis=0, tiled=True)
        d_w_out_part = lax.dot_general(hidden, d_out, (((0,), (0,)), ((), ())), preferred_element_type=f32)
        d_w_in_part = lax.dot_general(d_pre, normed, (((0,), (0,)), ((), ())), preferred_element_type=f32)
        d_w_part = jnp.concatenate([d_w_in_part.reshape(tp, hid, dim), d_w_out_part.reshape(tp, hid, dim)], axis=1)
        d_w = lax.psum_scatter(d_w_part.reshape(tp * 2 * hid, dim), "tp", scatter_dimension=0, tiled=True)
        d_w_in = d_w[:hid].T
        d_w_out = d_w[hid:]
        place = (lax.broadcasted_iota(jnp.int32, (vocab_local, token_ids.shape[0]), 0) == local_ids[None, :]).astype(bf16)
        d_table = jnp.dot(place, d_emb_full, preferred_element_type=f32)
        return block_out, d_table, d_w_in, d_w_out

    return jax.shard_map(
        shard_step,
        mesh=mesh,
        in_specs=(P("dp"), P("tp", None), P(None), P(None, "tp"), P("tp", None), P(("dp", "tp"), None)),
        out_specs=(P(("dp", "tp"), None), P(("dp", "tp"), None), P("dp", "tp"), P(("dp", "tp"), None)),
        check_vma=False,
    )
```

```python
import functools
import math

import jax
import jax.numpy as jnp
from jax import lax
from jax.experimental import pallas as pl
from jax.experimental.pallas import tpu as pltpu
from jax.sharding import PartitionSpec as P

EPS = 1e-6
F32, BF16 = jnp.float32, jnp.bfloat16
NT = (((1,), (1,)), ((), ()))


def _dot(a, b):
    return jnp.dot(a, b, preferred_element_type=F32)


def _gelu_and_grad(u):
    k0, k1 = 0.7978845608028654, 0.044715
    u2 = u * u
    t = jnp.tanh(k0 * (u + k1 * (u2 * u)))
    cdf = 0.5 * (1.0 + t)
    grad = cdf + (0.5 * u) * (1.0 - t * t) * (k0 + (3.0 * k0 * k1) * u2)
    return u * cdf, grad


def _kernel(
    n, side, share, ids_hbm, emb_ref, gain_hbm, w_in_ref, w_out_ref, d_out_hbm,
    out_ref, d_tab, d_w_in_ref, d_w_out_ref,
    ids_ref, gain_ref, d_out_ref, emb, emb_sib, w1, w2, first, ring, x_buf, n_buf, nt_buf, dot_buf, y_buf, dn_buf,
    dw, dw_sib, dw_ring, dx,
    load_sem, emb_sem, w_send, w_recv, w_push, w_got, cast_send, cast_recv, look_send, look_recv,
    dw_push, dw_got, dw_send, dw_recv, dx_send, dx_recv, dx_push, dx_got,
):
    rank = lax.axis_index("tp")
    z, c = rank // 2, rank % 2
    peer = 2 * z + (1 - c)
    far = n // 2
    last = n - 1
    hops = (2 * lax.rem(z + 1, n) + c, 2 * lax.rem(z + n - 1, n) + c)
    half, dim = first.shape[2], first.shape[3]
    v_rows, v_pad = emb_ref.shape[0], emb.shape[0]
    lane = ids_ref.shape[2]
    per_half = half // lane

    def send(src, dst, ssem, rsem, to):
        return pltpu.make_async_remote_copy(
            src_ref=src, dst_ref=dst, send_sem=ssem, recv_sem=rsem,
            device_id={"tp": to}, device_id_type=pl.DeviceIdType.MESH,
        )

    def chip(d, k):
        return lax.rem(z + (2 * d - 1) * k + 2 * n, n)

    loads = [
        pltpu.make_async_copy(src, dst, load_sem.at[i])
        for i, (src, dst) in enumerate(
            [
                (ids_hbm, ids_ref),
                (emb_ref, emb.at[pl.ds(0, v_rows)]),
                (w_in_ref, w1.at[rank]),
                (w_out_ref, w2.at[rank]),
                (d_out_hbm, d_out_ref),
                (gain_hbm, gain_ref),
            ]
        )
    ]
    for load in loads:
        load.start()
    emb[v_rows:] = jnp.zeros((v_pad - v_rows, dim), BF16)
    emb_sib[v_rows:] = jnp.zeros((v_pad - v_rows, dim), BF16)

    group = lax.axis_index("dp")
    gx, gy = group // side, group % side
    quarter = (2 * (gx % 2) + gy % 2) if share > 1 else 0
    square = []
    for e in range(1, share):
        px = gx + (e // 2) * (1 - 2 * (gx % 2))
        py = gy + (e % 2) * (1 - 2 * (gy % 2))
        square.append(px * side + py)

    barrier = pltpu.get_barrier_semaphore()
    for other in (*hops, peer):
        pl.semaphore_signal(barrier, inc=1, device_id={"tp": other}, device_id_type=pl.DeviceIdType.MESH)
    for other in square:
        pl.semaphore_signal(barrier, inc=1, device_id={"dp": other}, device_id_type=pl.DeviceIdType.MESH)
    pl.semaphore_wait(barrier, 2 + share)

    def w_part(w, ref):
        size = ref.shape[0] // share
        return ref.at[pl.ds(pl.multiple_of(quarter * size, size), size)]

    def w_block(w, d, m):
        return (w1, w2)[w].at[2 * chip(d, m) + c]

    def w_copy(d, m, w, own=False):
        dst = w_part(w, w_block(w, d, m))
        src = w_part(w, (w_in_ref, w_out_ref)[w]) if own else dst
        return send(src, dst, w_send.at[d, m, w], w_recv.at[d, m, w], hops[d])

    def w_casts(d, m, w):
        part = w_part(w, w_block(w, d, m))
        return [
            pltpu.make_async_remote_copy(
                src_ref=part, dst_ref=part,
                send_sem=cast_send.at[e, d, 2 * (m - 1) + w], recv_sem=cast_recv.at[e, d, 2 * (m - 1) + w],
                device_id={"dp": other}, device_id_type=pl.DeviceIdType.MESH,
            )
            for e, other in enumerate(square)
        ]

    def w_peer(d, m, w, own=False):
        dst = w_block(w, d, m)
        src = (w_in_ref, w_out_ref)[w] if own else dst
        return send(src, dst, w_push.at[d, m, w], w_got.at[d, m, w], peer)

    blocks = [(d, m, w) for m in range(1, far + 1) for d in range(2) for w in range(2) if m < far or w == d]

    def w_stage(m):
        for d, k, w in blocks:
            if k == m:
                w_copy(d, m - 1, w).wait_recv()
                if m < far - 1 or (m == far - 1 and w == d):
                    w_copy(d, m, w).start()
                for copy in w_casts(d, m, w):
                    copy.start()

    def w_share():
        for d, m, w in blocks:
            for copy in w_casts(d, m, w):
                copy.wait_recv()
            w_peer(d, m, w).start()

    emb_copy = send(emb_ref, emb_sib.at[pl.ds(0, v_rows)], emb_sem.at[0], emb_sem.at[1], peer)
    emb_copy.start()
    for d in range(2):
        for w in range(2):
            w_copy(d, 0, w, True).start()
    for w in range(2):
        w_peer(0, 0, w, True).start()

    lanes = lax.broadcasted_iota(jnp.int32, (2 * half, v_pad), 1)

    def wanted(j, h):
        at = (2 * (2 * j + c) + h) * per_half
        return [jnp.broadcast_to(ids_ref[at + i], (lane, lane)).T for i in range(per_half)]

    def pick(want, base):
        want = jnp.concatenate([want - base] * (v_pad // lane), axis=1)
        return jnp.where(want == lanes, 1.0, 0.0).astype(BF16)

    def look_half(d, p):
        return d + (1 - 2 * d) * (p % 2)

    def look_want(p):
        k = far - (p + 1) // 2
        return jnp.concatenate(
            [t for d in range(2) for t in wanted(chip(1 - d, k), look_half(d, p))], axis=0
        )

    def look_copy(d, p):
        return send(first.at[d, p], ring.at[d, p], look_send.at[d, p], look_recv.at[d, p], hops[d])

    def looked_up(want):
        return _dot(pick(want, rank * v_rows), emb[...]) + _dot(pick(want, peer * v_rows), emb_sib[...])

    loads[0].wait()
    loads[1].wait()
    want = look_want(0)
    x_buf[...] = _dot(pick(want, rank * v_rows), emb[...])
    w_stage(1)
    emb_copy.wait_recv()
    part = x_buf[...] + _dot(pick(want, peer * v_rows), emb_sib[...])
    for d in range(2):
        first[d, 0] = part[d * half : (d + 1) * half].astype(BF16)
        look_copy(d, 0).start()
    for load in loads[2:]:
        load.wait()

    def gather_round(p, carry):
        part = looked_up(look_want(p))
        for d in range(2):
            mine = part[d * half : (d + 1) * half]
            first[d, p] = mine.astype(BF16)

            @pl.when(p >= 2)
            def _():
                look_copy(d, p - 2).wait_recv()
                first[d, p] = (first[d, p].astype(F32) + ring[d, p - 2].astype(F32)).astype(BF16)

            look_copy(d, p).start()

        for at, m in ((1, 2), (3, 3), (5, 4)):

            @pl.when(p == at)
            def _():
                w_stage(m)

        @pl.when(p == last - 1)
        def _():
            w_share()

        return carry

    lax.fori_loop(1, last, gather_round, 0)
    x_buf[...] = looked_up(jnp.concatenate([t for h in range(2) for t in wanted(z, h)], axis=0))
    dot_buf[...] = d_out_ref[...].astype(F32).T.astype(BF16)
    y_buf[...] = jnp.zeros_like(y_buf)
    dn_buf[...] = jnp.zeros_like(dn_buf)
    for p in (last - 2, last - 1):
        for d in range(2):
            look_copy(d, p).wait_recv()

    x = x_buf[...] + jnp.concatenate(
        [ring[h, last - 1].astype(F32) + ring[1 - h, last - 2].astype(F32) for h in range(2)], axis=0
    )
    x_buf[...] = x
    inv_rms = lax.rsqrt(jnp.mean(x * x, axis=-1, keepdims=True) + EPS)
    gain = jnp.concatenate([gain_ref[i : i + 1].astype(F32) for i in range(gain_ref.shape[0])], axis=1)
    normed = (x * inv_rms * gain).astype(BF16)
    n_buf[...] = normed
    nt_buf[...] = normed.astype(F32).T.astype(BF16)

    def dw_peer(d, j):
        return send(dw.at[2 * j + (1 - c), d], dw_sib.at[j, d], dw_push.at[d, j], dw_got.at[d, j], peer)

    def dw_where(d, p):
        return chip(1 - d, far - (p + 1) // 2), look_half(d, p)

    def dw_copy(d, p):
        j, h = dw_where(d, p)
        return send(dw.at[2 * j + c, h], dw_ring.at[d, p], dw_send.at[d, p], dw_recv.at[d, p], hops[d])

    def dw_step(p, fresh=False):
        for d in range(2):
            j, h = dw_where(d, p)
            dw_peer(h, j).wait_recv()
            if fresh:
                dw[2 * j + c, h] = dw[2 * j + c, h] + dw_sib[j, h]
            else:
                dw_copy(d, p - 2).wait_recv()
                dw[2 * j + c, h] = (dw[2 * j + c, h] + dw_sib[j, h]) + dw_ring[d, p - 2]
            dw_copy(d, p).start()

    def tile_chip(i):
        return chip(i % 2, far - (i + 1) // 2)

    for d, m, w in blocks:
        w_peer(d, m, w).wait_recv()
    for w in range(2):
        w_peer(0, 0, w, True).wait_recv()

    def mlp(i, carry):
        j = tile_chip(i)
        w1t = jnp.concatenate([w1[2 * j], w1[2 * j + 1]], axis=1)
        w2t = jnp.concatenate([w2[2 * j], w2[2 * j + 1]], axis=0)
        hid = w1.shape[2]
        u = _dot(n_buf[...], w1t).astype(BF16).astype(F32)
        d_h = lax.dot_general(d_out_ref[...], w2t, NT, preferred_element_type=F32).astype(BF16).astype(F32)
        act, grad = _gelu_and_grad(u)
        h = act.astype(BF16)
        d_u = (d_h * grad).astype(BF16)
        y_buf[...] += _dot(h, w2t)
        dn_buf[...] += lax.dot_general(d_u, w1t, NT, preferred_element_type=F32)
        g1 = _dot(nt_buf[...], d_u)
        g2 = _dot(dot_buf[...], h)
        for q in range(2):
            dw[2 * j + q, 0] = g1[:, q * hid : (q + 1) * hid]
            dw[2 * j + q, 1] = g2[:, q * hid : (q + 1) * hid]

        for d in range(2):
            dw_peer(d, j).start()

        for at, p in ((1, 0), (3, 1)):

            @pl.when(i == at)
            def _():
                dw_step(p, fresh=True)

        return carry

    lax.fori_loop(0, n, mlp, 0)

    x = x_buf[...]
    d_scaled = dn_buf[...] * gain
    inv_rms = lax.rsqrt(jnp.mean(x * x, axis=-1, keepdims=True) + EPS)
    row_proj = jnp.mean(d_scaled * x, axis=-1, keepdims=True)
    dx[rank] = (
        d_out_ref[...].astype(F32) + inv_rms * (d_scaled - x * inv_rms * inv_rms * row_proj)
    ).astype(BF16)

    def dx_where(d, p):
        return chip(d, p // 2), d + (1 - 2 * d) * (p % 2)

    def dx_piece(d, p, core):
        j, h = dx_where(d, p)
        return dx.at[2 * j + core, pl.ds(pl.multiple_of(h * half, half), half)]

    def dx_copy(d, p):
        piece = dx_piece(d, p, c)
        return send(piece, piece, dx_send.at[d, p], dx_recv.at[d, p], hops[d])

    def dx_peer(d, p):
        piece = dx_piece(d, p, c)
        return send(piece, piece, dx_push.at[d, p], dx_got.at[d, p], peer)

    v_tile = v_pad // 4

    def add_rows(pieces, fresh=False):
        def tile(v, carry, size=v_tile):
            at = pl.ds(v * v_tile if isinstance(v, int) else pl.multiple_of(v * v_tile, v_tile), size)
            rows = lax.broadcasted_iota(jnp.int32, (size, half), 0)
            total = None if fresh else d_tab[at]
            for d, p, core in pieces:
                j, h = dx_where(d, p)
                i0 = (2 * (2 * j + core) + h) * per_half
                ids = jnp.concatenate([ids_ref[i0 + i] for i in range(per_half)], axis=1)
                place = jnp.where(rows == ids - (rank * v_rows + v * v_tile), 1.0, 0.0).astype(BF16)
                more = _dot(place, dx[2 * j + core, pl.ds(pl.multiple_of(h * half, half), half)])
                total = more if total is None else total + more
            d_tab[at] = total
            return carry

        lax.fori_loop(0, v_rows // v_tile, tile, 0)
        if v_rows % v_tile:
            tile(v_rows // v_tile, 0, v_rows % v_tile)

    for d in range(2):
        dx_copy(d, 0).start()
    for d in range(2):
        dx_copy(d, 1).start()
    for d in range(2):
        dx_peer(d, 0).start()
    out_ref[...] = (x + y_buf[...]).astype(BF16)
    add_rows([(0, 0, c), (1, 0, c)], fresh=True)

    def scatter_round(p, carry):
        for d in range(2):
            dx_copy(d, p - 2).wait_recv()
            dx_copy(d, p).start()
            dx_peer(d, p).start()

        @pl.when(p == 2)
        def _():
            for d in range(2):
                dx_peer(d, 0).wait_recv()

        @pl.when(p > 2)
        def _():
            for d in range(2):
                dx_peer(d, p - 1).wait_recv()

        was = p - 2 + (p + 1) // 4
        add_rows([(0, p, c), (1, p, c), (0, was, 1 - c), (1, was, 1 - c)])
        dw_step(p)
        return carry

    lax.fori_loop(2, last, scatter_round, 0)
    for p in (last, last + 1):
        for d in range(2):
            dx_copy(d, p - 2).wait_recv()
            dx_peer(d, p).start()
        for d in range(2):
            dx_peer(d, p - 1).wait_recv()
        add_rows([(0, p, c), (1, p, c), (0, p - 1, 1 - c), (1, p - 1, 1 - c)])
    for d in range(2):
        dx_peer(d, last + 1).wait_recv()
    add_rows([(0, last + 1, 1 - c), (1, last + 1, 1 - c)])
    sums = []
    for h in range(2):
        dw_peer(h, z).wait_recv()
        sums.append(dw[rank, h] + dw_sib[z, h])
    for d in range(2):
        dw_copy(d, last - 2).wait_recv()
    for d in range(2):
        dw_copy(d, last - 1).wait_recv()
    d_w_in_ref[...] = (sums[0] + dw_ring[1, last - 2]) + dw_ring[0, last - 1]
    d_w_out_ref[...] = ((sums[1] + dw_ring[0, last - 2]) + dw_ring[1, last - 1]).T

    emb_copy.wait_send()
    for d in range(2):
        for w in range(2):
            w_copy(d, 0, w, True).wait_send()
        dx_peer(d, 0).wait_send()
    for w in range(2):
        w_peer(0, 0, w, True).wait_send()
    for d, m, w in blocks:
        if m < far - 1 or (m == far - 1 and w == d):
            w_copy(d, m, w).wait_send()
        w_peer(d, m, w).wait_send()
        for copy in w_casts(d, m, w):
            copy.wait_send()

    def drain(k, carry):
        for d in range(2):
            dw_peer(d, k).wait_send()

            @pl.when(k < last)
            def _():
                look_copy(d, k).wait_send()
                dx_copy(d, k).wait_send()
                dw_copy(d, k).wait_send()

            @pl.when(k > 0)
            def _():
                dx_peer(d, k + 1).wait_send()

        return carry

    lax.fori_loop(0, n, drain, 0)


STORE_IN = pl.BlockSpec(memory_space=pl.ANY)


def _store(*refs):
    copies = [pltpu.make_async_copy(refs[i], refs[4 + i], refs[8].at[i]) for i in range(4)]
    for copy in copies:
        copy.start()
    for copy in copies:
        copy.wait()


def solution(mesh):
    tp = mesh.shape["tp"]
    n = tp // 2
    dp = mesh.shape["dp"]
    side = math.isqrt(dp)
    share = 4 if side * side == dp and side % 2 == 0 else 1

    def shard_step(token_ids, emb_table, norm_gain, w_in, w_out, d_out):
        v_rows, dim = emb_table.shape
        hid = w_out.shape[0]
        rows = d_out.shape[0]
        half = rows // 2
        lane = min(128, half)
        v_pad = -(-v_rows // 512) * 512
        vmem = pl.BlockSpec(memory_space=pltpu.VMEM)
        hbm = pl.BlockSpec(memory_space=pl.ANY)
        dma = pltpu.SemaphoreType.DMA
        results = pl.pallas_call(
            functools.partial(_kernel, n, side, share),
            out_shape=(
                pltpu.VMEM((rows, dim), BF16),
                pltpu.VMEM((v_rows, dim), F32),
                pltpu.VMEM((dim, hid), F32),
                pltpu.VMEM((hid, dim), F32),
            ),
            in_specs=[hbm] * 6,
            out_specs=(vmem,) * 4,
            scratch_shapes=[
                pltpu.VMEM((token_ids.shape[0] // lane, 1, lane), jnp.int32),
                pltpu.VMEM((dim // 128, 128), BF16),
                pltpu.VMEM((rows, dim), BF16),
                pltpu.VMEM((v_pad, dim), BF16),
                pltpu.VMEM((v_pad, dim), BF16),
                pltpu.VMEM((tp, dim, hid), BF16),
                pltpu.VMEM((tp, hid, dim), BF16),
                pltpu.VMEM((2, n - 1, half, dim), BF16),
                pltpu.VMEM((2, n - 1, half, dim), BF16),
                pltpu.VMEM((rows, dim), F32),
                pltpu.VMEM((rows, dim), BF16),
                pltpu.VMEM((dim, rows), BF16),
                pltpu.VMEM((dim, rows), BF16),
                pltpu.VMEM((rows, dim), F32),
                pltpu.VMEM((rows, dim), F32),
                pltpu.VMEM((tp, 2, dim, hid), F32),
                pltpu.VMEM((n, 2, dim, hid), F32),
                pltpu.VMEM((2, n - 1, dim, hid), F32),
                pltpu.VMEM((tp, rows, dim), BF16),
                dma((6,)),
                dma((2,)),
                dma((2, n // 2, 2)), dma((2, n // 2, 2)), dma((2, n // 2 + 1, 2)), dma((2, n // 2 + 1, 2)),
                dma((max(share - 1, 1), 2, n)), dma((max(share - 1, 1), 2, n)),
                dma((2, n - 1)), dma((2, n - 1)),
                dma((2, n)), dma((2, n)), dma((2, n - 1)), dma((2, n - 1)),
                dma((2, n - 1)), dma((2, n - 1)), dma((2, n + 1)), dma((2, n + 1)),
            ],
            compiler_params=pltpu.CompilerParams(
                collective_id=0, has_side_effects=True, vmem_limit_bytes=57 * 1024 * 1024
            ),
            name="block_step",
        )(token_ids.reshape(-1, 1, lane), emb_table, norm_gain.reshape(-1, 128), w_in, w_out, d_out)
        return pl.pallas_call(
            _store,
            out_shape=tuple(jax.ShapeDtypeStruct(r.shape, r.dtype) for r in results),
            in_specs=[STORE_IN] * 4,
            out_specs=(hbm,) * 4,
            scratch_shapes=[dma((4,))],
            compiler_params=pltpu.CompilerParams(vmem_limit_bytes=1024 * 1024),
            name="store",
        )(*results)

    return jax.shard_map(
        shard_step,
        mesh=mesh,
        in_specs=(P("dp"), P("tp", None), P(None), P(None, "tp"), P("tp", None), P(("dp", "tp"), None)),
        out_specs=(P(("dp", "tp"), None), P(("dp", "tp"), None), P("dp", "tp"), P(("dp", "tp"), None)),
        check_vma=False,
    )
```

```python
import functools
import math

import jax
import jax.numpy as jnp
from jax import lax
from jax.experimental import pallas as pl
from jax.experimental.pallas import tpu as pltpu
from jax.sharding import PartitionSpec as P

EPS = 1e-6
F32, BF16 = jnp.float32, jnp.bfloat16
NT = (((1,), (1,)), ((), ()))


def _dot(a, b):
    return jnp.dot(a, b, preferred_element_type=F32)


def _gelu_and_grad(u):
    k0, k1 = 0.7978845608028654, 0.044715
    u2 = u * u
    t = jnp.tanh(k0 * (u + k1 * (u2 * u)))
    cdf = 0.5 * (1.0 + t)
    grad = cdf + (0.5 * u) * (1.0 - t * t) * (k0 + (3.0 * k0 * k1) * u2)
    return u * cdf, grad


def _kernel(
    n, side, share, ids_hbm, emb_ref, gain_hbm, w_in_ref, w_out_ref, d_out_hbm,
    out_ref, d_tab, d_w_in_ref, d_w_out_ref,
    ids_ref, gain_ref, d_out_ref, emb, look_out, look_in, w1, w2, first, ring, x_buf, n_buf, nt_buf, dot_buf, y_buf, dn_buf,
    dw, dw_sib, dw_ring, dx,
    load_sem, w_send, w_recv, w_push, w_got, cast_send, cast_recv, look_send, look_recv, look_push, look_got,
    dw_push, dw_got, dw_send, dw_recv, dx_send, dx_recv, dx_push, dx_got,
):
    rank = lax.axis_index("tp")
    z, c = rank // 2, rank % 2
    peer = 2 * z + (1 - c)
    far = n // 2
    last = n - 1
    hops = (2 * lax.rem(z + 1, n) + c, 2 * lax.rem(z + n - 1, n) + c)
    half, dim = first.shape[2], first.shape[3]
    v_rows, v_pad = emb_ref.shape[0], emb.shape[0]
    lane = ids_ref.shape[2]
    per_half = half // lane

    def send(src, dst, ssem, rsem, to):
        return pltpu.make_async_remote_copy(
            src_ref=src, dst_ref=dst, send_sem=ssem, recv_sem=rsem,
            device_id={"tp": to}, device_id_type=pl.DeviceIdType.MESH,
        )

    def chip(d, k):
        return lax.rem(z + (2 * d - 1) * k + 2 * n, n)

    loads = [
        pltpu.make_async_copy(src, dst, load_sem.at[i])
        for i, (src, dst) in enumerate(
            [
                (ids_hbm, ids_ref),
                (emb_ref, emb.at[pl.ds(0, v_rows)]),
                (w_in_ref, w1.at[rank]),
                (w_out_ref, w2.at[rank]),
                (d_out_hbm, d_out_ref),
                (gain_hbm, gain_ref),
            ]
        )
    ]
    for load in loads:
        load.start()
    emb[v_rows:] = jnp.zeros((v_pad - v_rows, dim), BF16)

    group = lax.axis_index("dp")
    gx, gy = group // side, group % side
    quarter = (2 * (gx % 2) + gy % 2) if share > 1 else 0
    square = []
    for e in range(1, share):
        px = gx + (e // 2) * (1 - 2 * (gx % 2))
        py = gy + (e % 2) * (1 - 2 * (gy % 2))
        square.append(px * side + py)

    barrier = pltpu.get_barrier_semaphore()
    for other in (*hops, peer):
        pl.semaphore_signal(barrier, inc=1, device_id={"tp": other}, device_id_type=pl.DeviceIdType.MESH)
    for other in square:
        pl.semaphore_signal(barrier, inc=1, device_id={"dp": other}, device_id_type=pl.DeviceIdType.MESH)
    def w_part(w, ref):
        size = ref.shape[0] // share
        return ref.at[pl.ds(pl.multiple_of(quarter * size, size), size)]

    def w_block(w, d, m):
        return (w1, w2)[w].at[2 * chip(d, m) + c]

    def w_copy(d, m, w, own=False):
        dst = w_part(w, w_block(w, d, m))
        src = w_part(w, (w_in_ref, w_out_ref)[w]) if own else dst
        return send(src, dst, w_send.at[d, m, w], w_recv.at[d, m, w], hops[d])

    def w_casts(d, m, w):
        part = w_part(w, w_block(w, d, m))
        return [
            pltpu.make_async_remote_copy(
                src_ref=part, dst_ref=part,
                send_sem=cast_send.at[e, d, 2 * (m - 1) + w], recv_sem=cast_recv.at[e, d, 2 * (m - 1) + w],
                device_id={"dp": other}, device_id_type=pl.DeviceIdType.MESH,
            )
            for e, other in enumerate(square)
        ]

    def w_peer(d, m, w, own=False):
        dst = w_block(w, d, m)
        src = (w_in_ref, w_out_ref)[w] if own else dst
        return send(src, dst, w_push.at[d, m, w], w_got.at[d, m, w], peer)

    blocks = [(d, m, w) for m in range(1, far + 1) for d in range(2) for w in range(2) if m < far or w == d]

    def w_stage(m):
        for d, k, w in blocks:
            if k == m:
                w_copy(d, m - 1, w).wait_recv()
                if m < far - 1 or (m == far - 1 and w == d):
                    w_copy(d, m, w).start()
                for copy in w_casts(d, m, w):
                    copy.start()

    def w_share():
        for d, m, w in blocks:
            for copy in w_casts(d, m, w):
                copy.wait_recv()
            w_peer(d, m, w).start()

    lanes = lax.broadcasted_iota(jnp.int32, (2 * half, v_pad), 1)

    def wanted(j, h, core):
        at = (2 * (2 * j + core) + h) * per_half
        return [jnp.broadcast_to(ids_ref[at + i], (lane, lane)).T for i in range(per_half)]

    def look_half(d, p):
        return d + (1 - 2 * d) * (p % 2)

    def looked_up(p, core):
        k = far - (p + 1) // 2
        want = jnp.concatenate(
            [t for d in range(2) for t in wanted(chip(1 - d, k), look_half(d, p), core)], axis=0
        )
        want = jnp.concatenate([want - rank * v_rows] * (v_pad // lane), axis=1)
        return _dot(jnp.where(want == lanes, 1.0, 0.0).astype(BF16), emb[...])

    def look_peer(slot):
        return send(look_out.at[slot], look_in.at[slot], look_push.at[slot], look_got.at[slot], peer)

    def for_peer(slot):
        part = looked_up(slot + slot // last, 1 - c).astype(BF16)
        for d in range(2):
            look_out[slot, d] = part[d * half : (d + 1) * half]

    def look_copy(d, p):
        return send(first.at[d, p], ring.at[d, p], look_send.at[d, p], look_recv.at[d, p], hops[d])

    loads[0].wait()
    loads[1].wait()
    for_peer(0)
    pl.semaphore_wait(barrier, 2 + share)
    look_peer(0).start()
    for d in range(2):
        for w in range(2):
            w_copy(d, 0, w, True).start()
    for w in range(2):
        w_peer(0, 0, w, True).start()
    x_buf[...] = looked_up(0, c)
    look_peer(0).wait_recv()
    for d in range(2):
        first[d, 0] = (x_buf[pl.ds(d * half, half)] + look_in[0, d].astype(F32)).astype(BF16)
        look_copy(d, 0).start()
    for_peer(1)
    look_peer(1).start()
    for load in loads[2:]:
        load.wait()

    def gather_round(p, carry):
        x_buf[...] = looked_up(p, c)
        for m in range(1, far + 1):

            @pl.when(p == m)
            def _():
                w_stage(m)

        look_peer(p).wait_recv()
        for d in range(2):
            first[d, p] = (x_buf[pl.ds(d * half, half)] + look_in[p, d].astype(F32)).astype(BF16)

            @pl.when(p >= 2)
            def _():
                look_copy(d, p - 2).wait_recv()
                first[d, p] = (first[d, p].astype(F32) + ring[d, p - 2].astype(F32)).astype(BF16)

            look_copy(d, p).start()

        @pl.when(p == far + 1)
        def _():
            w_share()

        for_peer(p + 1)
        look_peer(p + 1).start()
        return carry

    lax.fori_loop(1, last, gather_round, 0)
    x_buf[...] = looked_up(n, c)
    look_peer(last).wait_recv()
    x_buf[...] = x_buf[...] + jnp.concatenate([look_in[last, h] for h in range(2)], axis=0).astype(F32)
    dot_buf[...] = d_out_ref[...].astype(F32).T.astype(BF16)
    y_buf[...] = jnp.zeros_like(y_buf)
    dn_buf[...] = jnp.zeros_like(dn_buf)
    for p in (last - 2, last - 1):
        for d in range(2):
            look_copy(d, p).wait_recv()

    x = x_buf[...] + jnp.concatenate(
        [ring[h, last - 1].astype(F32) + ring[1 - h, last - 2].astype(F32) for h in range(2)], axis=0
    )
    x_buf[...] = x
    inv_rms = lax.rsqrt(jnp.mean(x * x, axis=-1, keepdims=True) + EPS)
    gain = jnp.concatenate([gain_ref[i : i + 1].astype(F32) for i in range(gain_ref.shape[0])], axis=1)
    normed = (x * inv_rms * gain).astype(BF16)
    n_buf[...] = normed
    nt_buf[...] = normed.astype(F32).T.astype(BF16)

    def dw_peer(d, j):
        return send(dw.at[2 * j + (1 - c), d], dw_sib.at[j, d], dw_push.at[d, j], dw_got.at[d, j], peer)

    def dw_where(d, p):
        return chip(1 - d, far - (p + 1) // 2), look_half(d, p)

    def dw_copy(d, p):
        j, h = dw_where(d, p)
        return send(dw.at[2 * j + c, h], dw_ring.at[d, p], dw_send.at[d, p], dw_recv.at[d, p], hops[d])

    def dw_step(p, fresh=False):
        for d in range(2):
            j, h = dw_where(d, p)
            dw_peer(h, j).wait_recv()
            if fresh:
                dw[2 * j + c, h] = dw[2 * j + c, h] + dw_sib[j, h]
            else:
                dw_copy(d, p - 2).wait_recv()
                dw[2 * j + c, h] = (dw[2 * j + c, h] + dw_sib[j, h]) + dw_ring[d, p - 2]
            dw_copy(d, p).start()

    def tile_chip(i):
        return chip(i % 2, far - (i + 1) // 2)

    for d, m, w in blocks:
        w_peer(d, m, w).wait_recv()
    for w in range(2):
        w_peer(0, 0, w, True).wait_recv()

    def mlp(i, carry):
        j = tile_chip(i)
        w1t = jnp.concatenate([w1[2 * j], w1[2 * j + 1]], axis=1)
        w2t = jnp.concatenate([w2[2 * j], w2[2 * j + 1]], axis=0)
        hid = w1.shape[2]
        u = _dot(n_buf[...], w1t).astype(BF16).astype(F32)
        d_h = lax.dot_general(d_out_ref[...], w2t, NT, preferred_element_type=F32).astype(BF16).astype(F32)
        act, grad = _gelu_and_grad(u)
        h = act.astype(BF16)
        d_u = (d_h * grad).astype(BF16)
        y_buf[...] += _dot(h, w2t)
        dn_buf[...] += lax.dot_general(d_u, w1t, NT, preferred_element_type=F32)
        g1 = _dot(nt_buf[...], d_u)
        g2 = _dot(dot_buf[...], h)
        for q in range(2):
            dw[2 * j + q, 0] = g1[:, q * hid : (q + 1) * hid]
            dw[2 * j + q, 1] = g2[:, q * hid : (q + 1) * hid]

        for d in range(2):
            dw_peer(d, j).start()

        for at, p in ((1, 0), (3, 1)):

            @pl.when(i == at)
            def _():
                dw_step(p, fresh=True)

        return carry

    lax.fori_loop(0, n, mlp, 0)

    x = x_buf[...]
    d_scaled = dn_buf[...] * gain
    inv_rms = lax.rsqrt(jnp.mean(x * x, axis=-1, keepdims=True) + EPS)
    row_proj = jnp.mean(d_scaled * x, axis=-1, keepdims=True)
    dx[rank] = (
        d_out_ref[...].astype(F32) + inv_rms * (d_scaled - x * inv_rms * inv_rms * row_proj)
    ).astype(BF16)

    def dx_where(d, p):
        return chip(d, p // 2), d + (1 - 2 * d) * (p % 2)

    def dx_piece(d, p, core):
        j, h = dx_where(d, p)
        return dx.at[2 * j + core, pl.ds(pl.multiple_of(h * half, half), half)]

    def dx_copy(d, p):
        piece = dx_piece(d, p, c)
        return send(piece, piece, dx_send.at[d, p], dx_recv.at[d, p], hops[d])

    def dx_peer(d, p):
        piece = dx_piece(d, p, c)
        return send(piece, piece, dx_push.at[d, p], dx_got.at[d, p], peer)

    v_tile = v_pad // 4

    def add_rows(pieces, fresh=False):
        def tile(v, carry, size=v_tile):
            at = pl.ds(v * v_tile if isinstance(v, int) else pl.multiple_of(v * v_tile, v_tile), size)
            rows = lax.broadcasted_iota(jnp.int32, (size, half), 0)
            total = None if fresh else d_tab[at]
            for d, p, core in pieces:
                j, h = dx_where(d, p)
                i0 = (2 * (2 * j + core) + h) * per_half
                ids = jnp.concatenate([ids_ref[i0 + i] for i in range(per_half)], axis=1)
                place = jnp.where(rows == ids - (rank * v_rows + v * v_tile), 1.0, 0.0).astype(BF16)
                more = _dot(place, dx[2 * j + core, pl.ds(pl.multiple_of(h * half, half), half)])
                total = more if total is None else total + more
            d_tab[at] = total
            return carry

        lax.fori_loop(0, v_rows // v_tile, tile, 0)
        if v_rows % v_tile:
            tile(v_rows // v_tile, 0, v_rows % v_tile)

    for d in range(2):
        dx_copy(d, 0).start()
    for d in range(2):
        dx_copy(d, 1).start()
    for d in range(2):
        dx_peer(d, 0).start()
    out_ref[...] = (x + y_buf[...]).astype(BF16)
    add_rows([(0, 0, c), (1, 0, c)], fresh=True)

    def scatter_round(p, carry):
        for d in range(2):
            dx_copy(d, p - 2).wait_recv()
            dx_copy(d, p).start()
            dx_peer(d, p).start()

        @pl.when(p == 2)
        def _():
            for d in range(2):
                dx_peer(d, 0).wait_recv()

        @pl.when(p > 2)
        def _():
            for d in range(2):
                dx_peer(d, p - 1).wait_recv()

        was = p - 2 + (p + 1) // 4
        add_rows([(0, p, c), (1, p, c), (0, was, 1 - c), (1, was, 1 - c)])
        dw_step(p)
        return carry

    lax.fori_loop(2, last, scatter_round, 0)
    def finish(p):
        for d in range(2):
            dx_copy(d, p - 2).wait_recv()
            dx_peer(d, p).start()
        for d in range(2):
            dx_peer(d, p - 1).wait_recv()
        add_rows([(0, p, c), (1, p, c), (0, p - 1, 1 - c), (1, p - 1, 1 - c)])

    finish(last)

    for d in range(2):
        for w in range(2):
            w_copy(d, 0, w, True).wait_send()
        dx_peer(d, 0).wait_send()
    for w in range(2):
        w_peer(0, 0, w, True).wait_send()
    for d, m, w in blocks:
        if m < far - 1 or (m == far - 1 and w == d):
            w_copy(d, m, w).wait_send()
        w_peer(d, m, w).wait_send()
        for copy in w_casts(d, m, w):
            copy.wait_send()

    def drain(k, carry):
        look_peer(k).wait_send()
        for d in range(2):
            dw_peer(d, k).wait_send()

            @pl.when(k < last)
            def _():
                look_copy(d, k).wait_send()

            @pl.when(k < last - 2)
            def _():
                dx_copy(d, k).wait_send()
                dw_copy(d, k).wait_send()
                dx_peer(d, k + 2).wait_send()

        return carry

    lax.fori_loop(0, n, drain, 0)

    finish(last + 1)
    for d in range(2):
        dx_peer(d, last + 1).wait_recv()
    add_rows([(0, last + 1, 1 - c), (1, last + 1, 1 - c)])
    sums = []
    for h in range(2):
        dw_peer(h, z).wait_recv()
        sums.append(dw[rank, h] + dw_sib[z, h])
    for d in range(2):
        dw_copy(d, last - 2).wait_recv()
    for d in range(2):
        dw_copy(d, last - 1).wait_recv()
    d_w_in_ref[...] = (sums[0] + dw_ring[1, last - 2]) + dw_ring[0, last - 1]
    d_w_out_ref[...] = ((sums[1] + dw_ring[0, last - 2]) + dw_ring[1, last - 1]).T

    for d in range(2):
        for p in (last - 2, last - 1):
            dx_copy(d, p).wait_send()
            dw_copy(d, p).wait_send()
            dx_peer(d, p + 2).wait_send()


STORE_IN = pl.BlockSpec(memory_space=pl.ANY)


def _store(*refs):
    copies = [pltpu.make_async_copy(refs[i], refs[4 + i], refs[8].at[i]) for i in range(4)]
    for copy in copies:
        copy.start()
    for copy in copies:
        copy.wait()


def solution(mesh):
    tp = mesh.shape["tp"]
    n = tp // 2
    dp = mesh.shape["dp"]
    side = math.isqrt(dp)
    share = 4 if side * side == dp and side % 2 == 0 else 1

    def shard_step(token_ids, emb_table, norm_gain, w_in, w_out, d_out):
        v_rows, dim = emb_table.shape
        hid = w_out.shape[0]
        rows = d_out.shape[0]
        half = rows // 2
        lane = min(128, half)
        v_pad = -(-v_rows // 512) * 512
        vmem = pl.BlockSpec(memory_space=pltpu.VMEM)
        hbm = pl.BlockSpec(memory_space=pl.ANY)
        dma = pltpu.SemaphoreType.DMA
        results = pl.pallas_call(
            functools.partial(_kernel, n, side, share),
            out_shape=(
                pltpu.VMEM((rows, dim), BF16),
                pltpu.VMEM((v_rows, dim), F32),
                pltpu.VMEM((dim, hid), F32),
                pltpu.VMEM((hid, dim), F32),
            ),
            in_specs=[hbm] * 6,
            out_specs=(vmem,) * 4,
            scratch_shapes=[
                pltpu.VMEM((token_ids.shape[0] // lane, 1, lane), jnp.int32),
                pltpu.VMEM((dim // 128, 128), BF16),
                pltpu.VMEM((rows, dim), BF16),
                pltpu.VMEM((v_pad, dim), BF16),
                pltpu.VMEM((n, 2, half, dim), BF16),
                pltpu.VMEM((n, 2, half, dim), BF16),
                pltpu.VMEM((tp, dim, hid), BF16),
                pltpu.VMEM((tp, hid, dim), BF16),
                pltpu.VMEM((2, n - 1, half, dim), BF16),
                pltpu.VMEM((2, n - 1, half, dim), BF16),
                pltpu.VMEM((rows, dim), F32),
                pltpu.VMEM((rows, dim), BF16),
                pltpu.VMEM((dim, rows), BF16),
                pltpu.VMEM((dim, rows), BF16),
                pltpu.VMEM((rows, dim), F32),
                pltpu.VMEM((rows, dim), F32),
                pltpu.VMEM((tp, 2, dim, hid), F32),
                pltpu.VMEM((n, 2, dim, hid), F32),
                pltpu.VMEM((2, n - 1, dim, hid), F32),
                pltpu.VMEM((tp, rows, dim), BF16),
                dma((6,)),
                dma((2, n // 2, 2)), dma((2, n // 2, 2)), dma((2, n // 2 + 1, 2)), dma((2, n // 2 + 1, 2)),
                dma((max(share - 1, 1), 2, n)), dma((max(share - 1, 1), 2, n)),
                dma((2, n - 1)), dma((2, n - 1)), dma((n,)), dma((n,)),
                dma((2, n)), dma((2, n)), dma((2, n - 1)), dma((2, n - 1)),
                dma((2, n - 1)), dma((2, n - 1)), dma((2, n + 1)), dma((2, n + 1)),
            ],
            compiler_params=pltpu.CompilerParams(
                collective_id=0, has_side_effects=True, vmem_limit_bytes=57 * 1024 * 1024
            ),
            name="block_step",
        )(token_ids.reshape(-1, 1, lane), emb_table, norm_gain.reshape(-1, 128), w_in, w_out, d_out)
        return pl.pallas_call(
            _store,
            out_shape=tuple(jax.ShapeDtypeStruct(r.shape, r.dtype) for r in results),
            in_specs=[STORE_IN] * 4,
            out_specs=(hbm,) * 4,
            scratch_shapes=[dma((4,))],
            compiler_params=pltpu.CompilerParams(vmem_limit_bytes=1024 * 1024),
            name="store",
        )(*results)

    return jax.shard_map(
        shard_step,
        mesh=mesh,
        in_specs=(P("dp"), P("tp", None), P(None), P(None, "tp"), P("tp", None), P(("dp", "tp"), None)),
        out_specs=(P(("dp", "tp"), None), P(("dp", "tp"), None), P("dp", "tp"), P(("dp", "tp"), None)),
        check_vma=False,
    )
```

```python
import functools
import math

import jax
import jax.numpy as jnp
from jax import lax
from jax.experimental import pallas as pl
from jax.experimental.pallas import tpu as pltpu
from jax.sharding import PartitionSpec as P

EPS = 1e-6
F32, BF16 = jnp.float32, jnp.bfloat16
NT = (((1,), (1,)), ((), ()))


def _dot(a, b):
    return jnp.dot(a, b, preferred_element_type=F32)


def _gelu_and_grad(u):
    k0, k1 = 0.7978845608028654, 0.044715
    u2 = u * u
    t = jnp.tanh(k0 * (u + k1 * (u2 * u)))
    cdf = 0.5 * (1.0 + t)
    grad = cdf + (0.5 * u) * (1.0 - t * t) * (k0 + (3.0 * k0 * k1) * u2)
    return u * cdf, grad


def _kernel(
    n, side, share, ids_hbm, emb_ref, gain_hbm, w_in_ref, w_out_ref, d_out_hbm,
    out_ref, d_tab, d_w_in_ref, d_w_out_ref,
    ids_ref, gain_ref, d_out_ref, emb, look_out, look_in, w1, w2, first, ring, x_buf, n_buf, nt_buf, dot_buf, y_buf, dn_buf,
    dw, dw_sib, dw_ring, dx,
    load_sem, w_send, w_recv, w_push, w_got, cast_send, cast_recv, look_send, look_recv, look_push, look_got,
    dw_push, dw_got, dw_send, dw_recv, dx_send, dx_recv, dx_push, dx_got,
):
    rank = lax.axis_index("tp")
    z, c = rank // 2, rank % 2
    peer = 2 * z + (1 - c)
    far = n // 2
    last = n - 1
    hops = (2 * lax.rem(z + 1, n) + c, 2 * lax.rem(z + n - 1, n) + c)
    half, dim = first.shape[2], first.shape[3]
    v_rows, v_pad = emb_ref.shape[0], emb.shape[0]
    lane = ids_ref.shape[2]
    per_half = half // lane

    def send(src, dst, ssem, rsem, to):
        return pltpu.make_async_remote_copy(
            src_ref=src, dst_ref=dst, send_sem=ssem, recv_sem=rsem,
            device_id={"tp": to}, device_id_type=pl.DeviceIdType.MESH,
        )

    def chip(d, k):
        return lax.rem(z + (2 * d - 1) * k + 2 * n, n)

    loads = [
        pltpu.make_async_copy(src, dst, load_sem.at[i])
        for i, (src, dst) in enumerate(
            [
                (ids_hbm, ids_ref),
                (emb_ref, emb.at[pl.ds(0, v_rows)]),
                (w_in_ref, w1.at[rank]),
                (w_out_ref, w2.at[rank]),
                (d_out_hbm, d_out_ref),
                (gain_hbm, gain_ref),
            ]
        )
    ]
    for load in loads:
        load.start()
    emb[v_rows:] = jnp.zeros((v_pad - v_rows, dim), BF16)

    group = lax.axis_index("dp")
    gx, gy = group // side, group % side
    quarter = (2 * (gx % 2) + gy % 2) if share > 1 else 0
    square = []
    for e in range(1, share):
        px = gx + (e // 2) * (1 - 2 * (gx % 2))
        py = gy + (e % 2) * (1 - 2 * (gy % 2))
        square.append(px * side + py)

    barrier = pltpu.get_barrier_semaphore()
    for other in (*hops, peer):
        pl.semaphore_signal(barrier, inc=1, device_id={"tp": other}, device_id_type=pl.DeviceIdType.MESH)
    for other in square:
        pl.semaphore_signal(barrier, inc=1, device_id={"dp": other}, device_id_type=pl.DeviceIdType.MESH)
    def w_part(w, ref):
        size = ref.shape[0] // share
        return ref.at[pl.ds(pl.multiple_of(quarter * size, size), size)]

    def w_block(w, d, m):
        return (w1, w2)[w].at[2 * chip(d, m) + c]

    def w_copy(d, m, w, own=False):
        dst = w_part(w, w_block(w, d, m))
        src = w_part(w, (w_in_ref, w_out_ref)[w]) if own else dst
        return send(src, dst, w_send.at[0], w_recv.at[d, m], hops[d])

    def w_casts(d, m, w):
        part = w_part(w, w_block(w, d, m))
        return [
            pltpu.make_async_remote_copy(
                src_ref=part, dst_ref=part,
                send_sem=cast_send.at[e], recv_sem=cast_recv.at[e],
                device_id={"dp": other}, device_id_type=pl.DeviceIdType.MESH,
            )
            for e, other in enumerate(square)
        ]

    def w_peer(d, m, w, own=False):
        dst = w_block(w, d, m)
        src = (w_in_ref, w_out_ref)[w] if own else dst
        return send(src, dst, w_push.at[0], w_got.at[0], peer)

    blocks = [(d, m, w) for m in range(1, far + 1) for d in range(2) for w in range(2) if m < far or w == d]

    def bulk(parts):
        rows = parts * w2.shape[1] // share
        return dx.at[0, pl.ds(0, rows)] if rows <= dx.shape[1] else w2.at[pl.ds(0, parts)]

    def w_stage(m):
        for d in range(2):
            came = bulk(2 if m < far else 1)
            send(came, came, w_send.at[0], w_recv.at[d, m - 1], hops[d]).wait_recv()
        for d, k, w in blocks:
            if k == m:
                if m < far - 1 or (m == far - 1 and w == d):
                    w_copy(d, m, w).start()
                for copy in w_casts(d, m, w):
                    copy.start()

    def w_share():
        for e in range(share - 1):
            send(bulk(2 * last), bulk(2 * last), cast_send.at[e], cast_recv.at[e], peer).wait_recv()
        for d, m, w in blocks:
            w_peer(d, m, w).start()

    lanes = lax.broadcasted_iota(jnp.int32, (2 * half, v_pad), 1)

    def wanted(j, h, core):
        at = (2 * (2 * j + core) + h) * per_half
        return [jnp.broadcast_to(ids_ref[at + i], (lane, lane)).T for i in range(per_half)]

    def look_half(d, p):
        if isinstance(p, int) and p == 0:
            return 1 - d
        return (p + 1) % 2 + d * (p // last)

    def looked_up(p, core):
        k = far - (p + 1) // 2
        want = jnp.concatenate(
            [t for d in range(2) for t in wanted(chip(1 - d, k), look_half(d, p), core)], axis=0
        )
        want = jnp.concatenate([want - rank * v_rows] * (v_pad // lane), axis=1)
        return _dot(jnp.where(want == lanes, 1.0, 0.0).astype(BF16), emb[...])

    def look_peer(slot):
        return send(look_out.at[slot], look_in.at[slot], look_push.at[0], look_got.at[slot], peer)

    def for_peer(slot):
        part = looked_up(slot, 1 - c).astype(BF16)
        for d in range(2):
            look_out[slot, d] = part[d * half : (d + 1) * half]

    def look_copy(d, p):
        return send(first.at[d, p], ring.at[d, p], look_send.at[0], look_recv.at[d, p], hops[d])

    loads[0].wait()
    loads[1].wait()
    for_peer(0)
    pl.semaphore_wait(barrier, 2 + share)
    look_peer(0).start()
    for d in range(2):
        for w in range(2):
            w_copy(d, 0, w, True).start()
    for w in range(2):
        w_peer(0, 0, w, True).start()
    x_buf[...] = looked_up(0, c)
    look_peer(0).wait_recv()
    for d in range(2):
        first[d, 0] = (x_buf[pl.ds(d * half, half)] + look_in[0, d].astype(F32)).astype(BF16)
        look_copy(d, 0).start()
    for_peer(1)
    look_peer(1).start()
    for load in loads[2:]:
        load.wait()

    def gather_round(p, carry):
        x_buf[...] = looked_up(p, c)
        for m in range(1, far + 1):

            @pl.when(p == m)
            def _():
                w_stage(m)

        look_peer(p).wait_recv()
        for d in range(2):
            first[d, p] = (x_buf[pl.ds(d * half, half)] + look_in[p, d].astype(F32)).astype(BF16)

            @pl.when(p > 2 if d else p >= 2)
            def _():
                look_copy(d, p - 2).wait_recv()
                first[d, p] = (first[d, p].astype(F32) + ring[d, p - 2].astype(F32)).astype(BF16)

            if d:

                @pl.when(p == 1)
                def _():
                    look_copy(d, 0).wait_recv()
                    first[d, p] = (first[d, p].astype(F32) + ring[d, 0].astype(F32)).astype(BF16)

            look_copy(d, p).start()

        @pl.when(p == far + 1)
        def _():
            w_share()

        for_peer(p + 1)
        look_peer(p + 1).start()
        return carry

    lax.fori_loop(1, last, gather_round, 0)
    x_buf[...] = looked_up(last, c)
    look_peer(last).wait_recv()
    x_buf[...] = x_buf[...] + jnp.concatenate([look_in[last, h] for h in range(2)], axis=0).astype(F32)
    for h in range(2):
        dot_buf[h] = d_out_ref[pl.ds(h * half, half)].astype(F32).T.astype(BF16)
    y_buf[...] = jnp.zeros_like(y_buf)
    dn_buf[...] = jnp.zeros_like(dn_buf)
    gain = jnp.concatenate([gain_ref[i : i + 1].astype(F32) for i in range(gain_ref.shape[0])], axis=1)

    def norm(h):
        p = last - 2 + h
        at = pl.ds(h * half, half)
        for d in range(2):
            look_copy(d, p).wait_recv()
        x = x_buf[at] + (ring[0, p].astype(F32) + ring[1, p].astype(F32))
        x_buf[at] = x
        normed = (x * lax.rsqrt(jnp.mean(x * x, axis=-1, keepdims=True) + EPS) * gain).astype(BF16)
        n_buf[at] = normed
        nt_buf[h] = normed.astype(F32).T.astype(BF16)

    def dw_peer(d, j):
        return send(dw.at[2 * j + (1 - c), d], dw_sib.at[j, d], dw_push.at[0], dw_got.at[d, j], peer)

    def dw_where(d, p):
        return chip(1 - d, far - (p + 1) // 2), d + (1 - 2 * d) * (p % 2)

    def dw_copy(d, p):
        j, h = dw_where(d, p)
        return send(dw.at[2 * j + c, h], dw_ring.at[d, p], dw_send.at[0], dw_recv.at[d, p], hops[d])

    def dw_step(p, fresh=False, ways=(0, 1)):
        for d in ways:
            j, h = dw_where(d, p)
            dw_peer(h, j).wait_recv()
            if fresh:
                dw[2 * j + c, h] = dw[2 * j + c, h] + dw_sib[j, h]
            else:
                dw_copy(d, p - 2).wait_recv()
                dw[2 * j + c, h] = (dw[2 * j + c, h] + dw_sib[j, h]) + dw_ring[d, p - 2]
            dw_copy(d, p).start()

    def tile_chip(i):
        return chip(i % 2, far - (i + 1) // 2)

    send(w1, w1, w_push.at[0], w_got.at[0], peer).wait_recv()

    def mlp(i, h):
        at = pl.ds(h * half, half)
        j = tile_chip(i)
        w1t = jnp.concatenate([w1[2 * j], w1[2 * j + 1]], axis=1)
        w2t = jnp.concatenate([w2[2 * j], w2[2 * j + 1]], axis=0)
        hid = w1.shape[2]
        u = _dot(n_buf[at], w1t).astype(BF16).astype(F32)
        d_h = lax.dot_general(d_out_ref[at], w2t, NT, preferred_element_type=F32).astype(BF16).astype(F32)
        act, grad = _gelu_and_grad(u)
        hidden = act.astype(BF16)
        d_u = (d_h * grad).astype(BF16)
        y_buf[at] += _dot(hidden, w2t)
        dn_buf[at] += lax.dot_general(d_u, w1t, NT, preferred_element_type=F32)
        for which, g in ((0, _dot(nt_buf[h], d_u)), (1, _dot(dot_buf[h], hidden))):
            for q in range(2):
                piece = g[:, q * hid : (q + 1) * hid]
                dw[2 * j + q, which] = piece if h == 0 else dw[2 * j + q, which] + piece

    def first_half(i, carry):
        mlp(i, 0)
        return carry

    def second_half(i, carry):
        mlp(i, 1)
        for d in range(2):
            dw_peer(d, tile_chip(i)).start()

        for at, p in ((1, 0), (3, 1)):

            @pl.when(i == at)
            def _():
                dw_step(p, fresh=True)

        return carry

    def leave(h):
        at = pl.ds(h * half, half)
        x = x_buf[at]
        d_scaled = dn_buf[at] * gain
        inv_rms = lax.rsqrt(jnp.mean(x * x, axis=-1, keepdims=True) + EPS)
        row_proj = jnp.mean(d_scaled * x, axis=-1, keepdims=True)
        dx[rank, at] = (
            d_out_ref[at].astype(F32) + inv_rms * (d_scaled - x * inv_rms * inv_rms * row_proj)
        ).astype(BF16)
        for d in range(2):
            dx_copy(d, h).start()
        dx_peer(h, h).start()
        out_ref[at] = (x + y_buf[at]).astype(BF16)

    def dx_where(d, p):
        return chip(d, p // 2), p % 2 + d * (p // n)

    def dx_piece(d, p, core):
        j, h = dx_where(d, p)
        return dx.at[2 * j + core, pl.ds(pl.multiple_of(h * half, half), half)]

    def dx_copy(d, p):
        piece = dx_piece(d, p + d * (p // (last - 1)), c)
        return send(piece, piece, dx_send.at[0], dx_recv.at[d, p], hops[d])

    def dx_peer(d, p):
        piece = dx_piece(d, p, c)
        return send(piece, piece, dx_push.at[0], dx_got.at[d, p], peer)

    v_tile = v_pad // 4

    def add_rows(pieces, fresh=False):
        def tile(v, carry, size=v_tile):
            at = pl.ds(v * v_tile if isinstance(v, int) else pl.multiple_of(v * v_tile, v_tile), size)
            rows = lax.broadcasted_iota(jnp.int32, (size, half), 0)
            total = None if fresh else d_tab[at]
            for d, p, core in pieces:
                j, h = dx_where(d, p)
                i0 = (2 * (2 * j + core) + h) * per_half
                ids = jnp.concatenate([ids_ref[i0 + i] for i in range(per_half)], axis=1)
                place = jnp.where(rows == ids - (rank * v_rows + v * v_tile), 1.0, 0.0).astype(BF16)
                more = _dot(place, dx[2 * j + core, pl.ds(pl.multiple_of(h * half, half), half)])
                total = more if total is None else total + more
            d_tab[at] = total
            return carry

        lax.fori_loop(0, v_rows // v_tile, tile, 0)
        if v_rows % v_tile:
            tile(v_rows // v_tile, 0, v_rows % v_tile)

    norm(0)
    lax.fori_loop(0, n, first_half, 0)
    leave(0)
    norm(1)
    lax.fori_loop(0, n, second_half, 0)
    leave(1)
    dw_step(2)
    add_rows([(0, 0, c), (0, 1, c)], fresh=True)

    def scatter_round(p, carry):
        for d in range(2):
            dx_copy(d, p - 2).wait_recv()
            dx_copy(d, p).start()
            dx_peer(d, p).start()

        @pl.when(p == 2)
        def _():
            for d in range(2):
                dx_peer(d, d).wait_recv()

        @pl.when(p > 2)
        def _():
            for d in range(2):
                dx_peer(d, p - 1).wait_recv()

        add_rows([(0, p, c), (1, p, c), (0, (p - 1) * ((p + 1) // 4), 1 - c), (1, p - 1, 1 - c)])

        @pl.when(p > 2)
        def _():
            dw_step(p)

        return carry

    lax.fori_loop(2, last - 1, scatter_round, 0)

    def finish(p, ways):
        for d in range(2):
            dx_copy(d, p - 2).wait_recv()
            if d in ways:
                dx_copy(d, last - 1).start()
            dx_peer(d, p).start()
        for d in range(2):
            dx_peer(d, p - 1).wait_recv()
        add_rows([(0, p, c), (1, p, c), (0, p - 1, 1 - c), (1, p - 1, 1 - c)])
        if ways:
            dw_step(last - 1, ways=ways)

    finish(last - 1, (0,))
    finish(last, (1,))
    finish(last + 1, ())
    for d in range(2):
        dx_peer(d, last + 1).wait_recv()
    add_rows([(0, last + 1, 1 - c), (1, last + 1, 1 - c)])
    sums = []
    for h in range(2):
        dw_peer(h, z).wait_recv()
        sums.append(dw[rank, h] + dw_sib[z, h])
    for d in range(2):
        dw_copy(d, last - 2).wait_recv()
    for d in range(2):
        dw_copy(d, last - 1).wait_recv()
    d_w_in_ref[...] = (sums[0] + dw_ring[1, last - 2]) + dw_ring[0, last - 1]
    d_w_out_ref[...] = ((sums[1] + dw_ring[0, last - 2]) + dw_ring[1, last - 1]).T

    for copy in (
        send(first, ring, look_send.at[0], look_recv.at[0, 0], peer),
        send(look_out, look_in, look_push.at[0], look_got.at[0], peer),
        send(w1, w1, w_push.at[0], w_got.at[0], peer),
        send(dw_sib, dw_sib, dw_push.at[0], dw_got.at[0, 0], peer),
        send(dw_ring, dw_ring, dw_send.at[0], dw_recv.at[0, 0], peer),
        send(ring, ring, dx_send.at[0], dx_recv.at[0, 0], peer),
        send(look_in, look_in, dx_push.at[0], dx_got.at[0, 0], peer),
        send(bulk(2 * last), bulk(2 * last), w_send.at[0], w_recv.at[0, 0], peer),
        *[send(bulk(2 * last), bulk(2 * last), cast_send.at[e], cast_recv.at[e], peer) for e in range(share - 1)],
    ):
        copy.wait_send()


STORE_IN = pl.BlockSpec(memory_space=pl.ANY)


def _store(*refs):
    copies = [pltpu.make_async_copy(refs[i], refs[4 + i], refs[8].at[i]) for i in range(4)]
    for copy in copies:
        copy.start()
    for copy in copies:
        copy.wait()


def solution(mesh):
    tp = mesh.shape["tp"]
    n = tp // 2
    dp = mesh.shape["dp"]
    side = math.isqrt(dp)
    share = 4 if side * side == dp and side % 2 == 0 else 1

    def shard_step(token_ids, emb_table, norm_gain, w_in, w_out, d_out):
        v_rows, dim = emb_table.shape
        hid = w_out.shape[0]
        rows = d_out.shape[0]
        half = rows // 2
        lane = min(128, half)
        v_pad = -(-v_rows // 512) * 512
        vmem = pl.BlockSpec(memory_space=pltpu.VMEM)
        hbm = pl.BlockSpec(memory_space=pl.ANY)
        dma = pltpu.SemaphoreType.DMA
        results = pl.pallas_call(
            functools.partial(_kernel, n, side, share),
            out_shape=(
                pltpu.VMEM((rows, dim), BF16),
                pltpu.VMEM((v_rows, dim), F32),
                pltpu.VMEM((dim, hid), F32),
                pltpu.VMEM((hid, dim), F32),
            ),
            in_specs=[hbm] * 6,
            out_specs=(vmem,) * 4,
            scratch_shapes=[
                pltpu.VMEM((token_ids.shape[0] // lane, 1, lane), jnp.int32),
                pltpu.VMEM((dim // 128, 128), BF16),
                pltpu.VMEM((rows, dim), BF16),
                pltpu.VMEM((v_pad, dim), BF16),
                pltpu.VMEM((n, 2, half, dim), BF16),
                pltpu.VMEM((n, 2, half, dim), BF16),
                pltpu.VMEM((tp, dim, hid), BF16),
                pltpu.VMEM((tp, hid, dim), BF16),
                pltpu.VMEM((2, n - 1, half, dim), BF16),
                pltpu.VMEM((2, n - 1, half, dim), BF16),
                pltpu.VMEM((rows, dim), F32),
                pltpu.VMEM((rows, dim), BF16),
                pltpu.VMEM((2, dim, half), BF16),
                pltpu.VMEM((2, dim, half), BF16),
                pltpu.VMEM((rows, dim), F32),
                pltpu.VMEM((rows, dim), F32),
                pltpu.VMEM((tp, 2, dim, hid), F32),
                pltpu.VMEM((n, 2, dim, hid), F32),
                pltpu.VMEM((2, n - 1, dim, hid), F32),
                pltpu.VMEM((tp, rows, dim), BF16),
                dma((6,)),
                dma((1,)), dma((2, n // 2)), dma((1,)), dma((1,)),
                dma((max(share - 1, 1),)), dma((max(share - 1, 1),)),
                dma((1,)), dma((2, n - 1)), dma((1,)), dma((n,)),
                dma((1,)), dma((2, n)), dma((1,)), dma((2, n - 1)),
                dma((1,)), dma((2, n - 1)), dma((1,)), dma((2, n + 1)),
            ],
            compiler_params=pltpu.CompilerParams(
                collective_id=0, has_side_effects=True, vmem_limit_bytes=57 * 1024 * 1024
            ),
            name="block_step",
        )(token_ids.reshape(-1, 1, lane), emb_table, norm_gain.reshape(-1, 128), w_in, w_out, d_out)
        return pl.pallas_call(
            _store,
            out_shape=tuple(jax.ShapeDtypeStruct(r.shape, r.dtype) for r in results),
            in_specs=[STORE_IN] * 4,
            out_specs=(hbm,) * 4,
            scratch_shapes=[dma((4,))],
            compiler_params=pltpu.CompilerParams(vmem_limit_bytes=1024 * 1024),
            name="store",
        )(*results)

    return jax.shard_map(
        shard_step,
        mesh=mesh,
        in_specs=(P("dp"), P("tp", None), P(None), P(None, "tp"), P("tp", None), P(("dp", "tp"), None)),
        out_specs=(P(("dp", "tp"), None), P(("dp", "tp"), None), P("dp", "tp"), P(("dp", "tp"), None)),
        check_vma=False,
    )
```

```python
import functools
import math

import jax
import jax.numpy as jnp
from jax import lax
from jax.experimental import pallas as pl
from jax.experimental.pallas import tpu as pltpu
from jax.sharding import PartitionSpec as P

EPS = 1e-6
F32, BF16 = jnp.float32, jnp.bfloat16
NT = (((1,), (1,)), ((), ()))


def _dot(a, b):
    return jnp.dot(a, b, preferred_element_type=F32)


def _gelu_and_grad(u):
    k0, k1 = 0.7978845608028654, 0.044715
    u2 = u * u
    t = jnp.tanh(k0 * (u + k1 * (u2 * u)))
    cdf = 0.5 * (1.0 + t)
    grad = cdf + (0.5 * u) * (1.0 - t * t) * (k0 + (3.0 * k0 * k1) * u2)
    return u * cdf, grad


def _kernel(
    n, side, share, ids_hbm, emb_ref, gain_hbm, w_in_ref, w_out_ref, d_out_hbm,
    out_ref, d_tab, d_w_in_ref, d_w_out_ref,
    ids_ref, gain_ref, d_out_ref, emb, look_out, look_in, w1, w2, first, ring, x_buf, n_buf, nt_buf, dot_buf, dh_buf, h_buf, du_buf, y_buf, dn_buf,
    dw, dw_sib, dw_ring, dx,
    load_sem, w_send, w_recv, w_push, w_got, cast_send, cast_recv, look_send, look_recv, look_push, look_got,
    dw_push, dw_got, dw_send, dw_recv, dx_send, dx_recv, dx_push, dx_got,
):
    rank = lax.axis_index("tp")
    z, c = rank // 2, rank % 2
    peer = 2 * z + (1 - c)
    far = n // 2
    last = n - 1
    hops = (2 * lax.rem(z + 1, n) + c, 2 * lax.rem(z + n - 1, n) + c)
    half, dim = first.shape[2], first.shape[3]
    v_rows, v_pad = emb_ref.shape[0], emb.shape[0]
    lane = ids_ref.shape[2]
    per_half = half // lane

    def send(src, dst, ssem, rsem, to):
        return pltpu.make_async_remote_copy(
            src_ref=src, dst_ref=dst, send_sem=ssem, recv_sem=rsem,
            device_id={"tp": to}, device_id_type=pl.DeviceIdType.MESH,
        )

    def chip(d, k):
        return lax.rem(z + (2 * d - 1) * k + 2 * n, n)

    loads = [
        pltpu.make_async_copy(src, dst, load_sem.at[i])
        for i, (src, dst) in enumerate(
            [
                (ids_hbm, ids_ref),
                (emb_ref, emb.at[pl.ds(0, v_rows)]),
                (w_in_ref, w1.at[rank]),
                (w_out_ref, w2.at[rank]),
                (d_out_hbm, d_out_ref),
                (gain_hbm, gain_ref),
            ]
        )
    ]
    for load in loads:
        load.start()
    emb[v_rows:] = jnp.zeros((v_pad - v_rows, dim), BF16)

    group = lax.axis_index("dp")
    gx, gy = group // side, group % side
    quarter = (2 * (gx % 2) + gy % 2) if share > 1 else 0
    square = []
    for e in range(1, share):
        px = gx + (e // 2) * (1 - 2 * (gx % 2))
        py = gy + (e % 2) * (1 - 2 * (gy % 2))
        square.append(px * side + py)

    barrier = pltpu.get_barrier_semaphore()
    for other in (*hops, peer):
        pl.semaphore_signal(barrier, inc=1, device_id={"tp": other}, device_id_type=pl.DeviceIdType.MESH)
    for other in square:
        pl.semaphore_signal(barrier, inc=1, device_id={"dp": other}, device_id_type=pl.DeviceIdType.MESH)
    def w_part(w, ref):
        size = ref.shape[0] // share
        return ref.at[pl.ds(pl.multiple_of(quarter * size, size), size)]

    def w_block(w, d, m):
        return (w1, w2)[w].at[2 * chip(d, m) + c]

    def w_copy(d, m, w, own=False):
        dst = w_part(w, w_block(w, d, m))
        src = w_part(w, (w_in_ref, w_out_ref)[w]) if own else dst
        return send(src, dst, w_send.at[0], w_recv.at[d, m], hops[d])

    def w_casts(d, m, w):
        part = w_part(w, w_block(w, d, m))
        return [
            pltpu.make_async_remote_copy(
                src_ref=part, dst_ref=part,
                send_sem=cast_send.at[e], recv_sem=cast_recv.at[e],
                device_id={"dp": other}, device_id_type=pl.DeviceIdType.MESH,
            )
            for e, other in enumerate(square)
        ]

    def w_peer(d, m, w, own=False):
        dst = w_block(w, d, m)
        src = (w_in_ref, w_out_ref)[w] if own else dst
        return send(src, dst, w_push.at[0], w_got.at[0], peer)

    blocks = [(d, m, w) for m in range(1, far + 1) for d in range(2) for w in range(2) if m < far or w == d]

    def bulk(parts):
        rows = parts * w2.shape[1] // share
        return dx.at[0, pl.ds(0, rows)] if rows <= dx.shape[1] else w2.at[pl.ds(0, parts)]

    def w_stage(m):
        for d in range(2):
            came = bulk(2 if m < far else 1)
            send(came, came, w_send.at[0], w_recv.at[d, m - 1], hops[d]).wait_recv()
        for d, k, w in blocks:
            if k == m:
                if m < far - 1 or (m == far - 1 and w == d):
                    w_copy(d, m, w).start()
                for copy in w_casts(d, m, w):
                    copy.start()

    def w_share():
        for e in range(share - 1):
            send(bulk(2 * last), bulk(2 * last), cast_send.at[e], cast_recv.at[e], peer).wait_recv()
        for d, m, w in blocks:
            w_peer(d, m, w).start()

    lanes = lax.broadcasted_iota(jnp.int32, (2 * half, v_pad), 1)

    def wanted(j, h, core):
        at = (2 * (2 * j + core) + h) * per_half
        return [jnp.broadcast_to(ids_ref[at + i], (lane, lane)).T for i in range(per_half)]

    def look_half(d, p):
        if isinstance(p, int) and p == 0:
            return 1 - d
        return (p + 1) % 2 + d * (p // last)

    def looked_up(p, core):
        k = far - (p + 1) // 2
        want = jnp.concatenate(
            [t for d in range(2) for t in wanted(chip(1 - d, k), look_half(d, p), core)], axis=0
        )
        want = jnp.concatenate([want - rank * v_rows] * (v_pad // lane), axis=1)
        return _dot(jnp.where(want == lanes, 1.0, 0.0).astype(BF16), emb[...])

    def look_peer(slot):
        return send(look_out.at[slot], look_in.at[slot], look_push.at[0], look_got.at[slot], peer)

    def for_peer(slot):
        part = looked_up(slot, 1 - c).astype(BF16)
        for d in range(2):
            look_out[slot, d] = part[d * half : (d + 1) * half]

    def look_copy(d, p):
        return send(first.at[d, p], ring.at[d, p], look_send.at[0], look_recv.at[d, p], hops[d])

    loads[0].wait()
    loads[1].wait()
    for_peer(0)
    pl.semaphore_wait(barrier, 2 + share)
    look_peer(0).start()
    x_buf[...] = looked_up(0, c)
    look_peer(0).wait_recv()
    for d in range(2):
        first[d, 0] = (x_buf[pl.ds(d * half, half)] + look_in[0, d].astype(F32)).astype(BF16)
        look_copy(d, 0).start()
    for d in range(2):
        for w in range(2):
            w_copy(d, 0, w, True).start()
    for_peer(1)
    look_peer(1).start()
    for w in range(2):
        w_peer(0, 0, w, True).start()
    for load in loads[2:]:
        load.wait()

    def gather_round(p, carry):
        x_buf[...] = looked_up(p, c)
        for m in range(1, far + 1):

            @pl.when(p == m + 1)
            def _():
                w_stage(m)

        look_peer(p).wait_recv()
        for d in range(2):
            first[d, p] = (x_buf[pl.ds(d * half, half)] + look_in[p, d].astype(F32)).astype(BF16)

            @pl.when(p > 2 if d else p >= 2)
            def _():
                look_copy(d, p - 2).wait_recv()
                first[d, p] = (first[d, p].astype(F32) + ring[d, p - 2].astype(F32)).astype(BF16)

            if d:

                @pl.when(p == 1)
                def _():
                    look_copy(d, 0).wait_recv()
                    first[d, p] = (first[d, p].astype(F32) + ring[d, 0].astype(F32)).astype(BF16)

            look_copy(d, p).start()

        @pl.when(p == last - 1)
        def _():
            w_share()

        for_peer(p + 1)
        look_peer(p + 1).start()
        return carry

    lax.fori_loop(1, last, gather_round, 0)
    x_buf[...] = looked_up(last, c)
    look_peer(last).wait_recv()
    x_buf[...] = x_buf[...] + jnp.concatenate([look_in[last, h] for h in range(2)], axis=0).astype(F32)
    dot_buf[...] = d_out_ref[...].astype(F32).T.astype(BF16)
    y_buf[...] = jnp.zeros_like(y_buf)
    dn_buf[...] = jnp.zeros_like(dn_buf)
    gain = jnp.concatenate([gain_ref[i : i + 1].astype(F32) for i in range(gain_ref.shape[0])], axis=1)

    def norm(h):
        p = last - 2 + h
        at = pl.ds(h * half, half)
        for d in range(2):
            look_copy(d, p).wait_recv()
        x = x_buf[at] + (ring[0, p].astype(F32) + ring[1, p].astype(F32))
        x_buf[at] = x
        normed = (x * lax.rsqrt(jnp.mean(x * x, axis=-1, keepdims=True) + EPS) * gain).astype(BF16)
        n_buf[at] = normed
        nt_buf[:, pl.ds(h * half, half)] = normed.astype(F32).T.astype(BF16)

    def dw_peer(d, j):
        return send(dw.at[2 * j + (1 - c), d], dw_sib.at[j, d], dw_push.at[0], dw_got.at[d, j], peer)

    def dw_where(d, p):
        return chip(1 - d, far - (p + 1) // 2), d + (1 - 2 * d) * (p % 2)

    def dw_copy(d, p):
        j, h = dw_where(d, p)
        return send(dw.at[2 * j + c, h], dw_ring.at[d, p], dw_send.at[0], dw_recv.at[d, p], hops[d])

    def dw_step(p, fresh=False, ways=(0, 1)):
        for d in ways:
            j, h = dw_where(d, p)
            dw_peer(h, j).wait_recv()
            if fresh:
                dw[2 * j + c, h] = dw[2 * j + c, h] + dw_sib[j, h]
            else:
                dw_copy(d, p - 2).wait_recv()
                dw[2 * j + c, h] = (dw[2 * j + c, h] + dw_sib[j, h]) + dw_ring[d, p - 2]
            dw_copy(d, p).start()

    def tile_chip(i):
        return chip(i % 2, far - (i + 1) // 2)

    send(w1, w1, w_push.at[0], w_got.at[0], peer).wait_recv()

    def weights(i):
        j = tile_chip(i)
        w1t = jnp.concatenate([w1[2 * j], w1[2 * j + 1]], axis=1)
        w2t = jnp.concatenate([w2[2 * j], w2[2 * j + 1]], axis=0)
        return j, w1t, w2t

    def hidden_grad(i, h):
        out_grad = d_out_ref[pl.ds(h * half, half)]
        return lax.dot_general(out_grad, weights(i)[2], NT, preferred_element_type=F32).astype(BF16)

    def early(i, carry):
        dh_buf[i] = hidden_grad(i, 0)
        return carry

    def inner(i, h, d_h):
        at = pl.ds(h * half, half)
        w1t = weights(i)[1]
        act, grad = _gelu_and_grad(_dot(n_buf[at], w1t).astype(BF16).astype(F32))
        hidden = act.astype(BF16)
        d_u = (d_h.astype(F32) * grad).astype(BF16)
        dn_buf[at] += lax.dot_general(d_u, w1t, NT, preferred_element_type=F32)
        return hidden, d_u

    def first_half(i, carry):
        h_buf[i], du_buf[i] = inner(i, 0, dh_buf[i])
        return carry

    def second_half(i, carry):
        j, _, w2t = weights(i)
        hid = w1.shape[2]
        hidden, d_u = inner(i, 1, hidden_grad(i, 1))
        hidden = jnp.concatenate([h_buf[i], hidden], axis=0)
        d_u = jnp.concatenate([du_buf[i], d_u], axis=0)
        for which, g in ((0, _dot(nt_buf[...], d_u)), (1, _dot(dot_buf[...], hidden))):
            for q in range(2):
                dw[2 * j + q, which] = g[:, q * hid : (q + 1) * hid]
        for d in range(2):
            dw_peer(d, j).start()
        y_buf[...] += _dot(hidden, w2t)

        for at, p in ((1, 0), (3, 1)):

            @pl.when(i == at)
            def _():
                dw_step(p, fresh=True)

        return carry

    def leave(h):
        at = pl.ds(h * half, half)
        x = x_buf[at]
        d_scaled = dn_buf[at] * gain
        inv_rms = lax.rsqrt(jnp.mean(x * x, axis=-1, keepdims=True) + EPS)
        row_proj = jnp.mean(d_scaled * x, axis=-1, keepdims=True)
        dx[rank, at] = (
            d_out_ref[at].astype(F32) + inv_rms * (d_scaled - x * inv_rms * inv_rms * row_proj)
        ).astype(BF16)
        for d in range(2):
            dx_copy(d, h).start()
        dx_peer(h, h).start()

    def dx_where(d, p):
        return chip(d, p // 2), p % 2 + d * (p // n)

    def dx_piece(d, p, core):
        j, h = dx_where(d, p)
        return dx.at[2 * j + core, pl.ds(pl.multiple_of(h * half, half), half)]

    def dx_copy(d, p):
        piece = dx_piece(d, p + d * (p // (last - 1)), c)
        return send(piece, piece, dx_send.at[0], dx_recv.at[d, p], hops[d])

    def dx_peer(d, p):
        piece = dx_piece(d, p, c)
        return send(piece, piece, dx_push.at[0], dx_got.at[d, p], peer)

    v_tile = v_pad // 4

    def add_rows(pieces, fresh=False):
        def tile(v, carry, size=v_tile):
            at = pl.ds(v * v_tile if isinstance(v, int) else pl.multiple_of(v * v_tile, v_tile), size)
            rows = lax.broadcasted_iota(jnp.int32, (size, half), 0)
            total = None if fresh else d_tab[at]
            for d, p, core in pieces:
                j, h = dx_where(d, p)
                i0 = (2 * (2 * j + core) + h) * per_half
                ids = jnp.concatenate([ids_ref[i0 + i] for i in range(per_half)], axis=1)
                place = jnp.where(rows == ids - (rank * v_rows + v * v_tile), 1.0, 0.0).astype(BF16)
                more = _dot(place, dx[2 * j + core, pl.ds(pl.multiple_of(h * half, half), half)])
                total = more if total is None else total + more
            d_tab[at] = total
            return carry

        lax.fori_loop(0, v_rows // v_tile, tile, 0)
        if v_rows % v_tile:
            tile(v_rows // v_tile, 0, v_rows % v_tile)

    lax.fori_loop(0, n, early, 0)
    norm(0)
    lax.fori_loop(0, n, first_half, 0)
    leave(0)
    norm(1)
    lax.fori_loop(0, n, second_half, 0)
    leave(1)
    out_ref[...] = (x_buf[...] + y_buf[...]).astype(BF16)
    dw_step(2)
    add_rows([(0, 0, c), (0, 1, c)], fresh=True)

    def scatter_round(p, carry):
        for d in range(2):
            dx_copy(d, p - 2).wait_recv()
            dx_copy(d, p).start()
            dx_peer(d, p).start()

        @pl.when(p == 2)
        def _():
            for d in range(2):
                dx_peer(d, d).wait_recv()

        @pl.when(p > 2)
        def _():
            for d in range(2):
                dx_peer(d, p - 1).wait_recv()

        add_rows([(0, p, c), (1, p, c), (0, (p - 1) * ((p + 1) // 4), 1 - c), (1, p - 1, 1 - c)])

        @pl.when(p > 2)
        def _():
            dw_step(p)

        return carry

    lax.fori_loop(2, last - 1, scatter_round, 0)

    def finish(p, ways):
        for d in range(2):
            dx_peer(d, p - 1).wait_recv()
        add_rows([(0, p - 1, 1 - c), (1, p - 1, 1 - c)])
        for d in range(2):
            dx_copy(d, p - 2).wait_recv()
            if d in ways:
                dx_copy(d, last - 1).start()
            dx_peer(d, p).start()
        add_rows([(0, p, c), (1, p, c)])
        if ways:
            dw_step(last - 1, ways=ways)

    finish(last - 1, (0,))
    finish(last, (1,))
    finish(last + 1, ())
    for d in range(2):
        dx_peer(d, last + 1).wait_recv()
    add_rows([(0, last + 1, 1 - c), (1, last + 1, 1 - c)])
    sums = []
    for h in range(2):
        dw_peer(h, z).wait_recv()
        sums.append(dw[rank, h] + dw_sib[z, h])
    for d in range(2):
        dw_copy(d, last - 2).wait_recv()
    for d in range(2):
        dw_copy(d, last - 1).wait_recv()
    d_w_in_ref[...] = (sums[0] + dw_ring[1, last - 2]) + dw_ring[0, last - 1]
    d_w_out_ref[...] = ((sums[1] + dw_ring[0, last - 2]) + dw_ring[1, last - 1]).T

    for copy in (
        send(first, ring, look_send.at[0], look_recv.at[0, 0], peer),
        send(look_out, look_in, look_push.at[0], look_got.at[0], peer),
        send(w1, w1, w_push.at[0], w_got.at[0], peer),
        send(dw_sib, dw_sib, dw_push.at[0], dw_got.at[0, 0], peer),
        send(dw_ring, dw_ring, dw_send.at[0], dw_recv.at[0, 0], peer),
        send(ring, ring, dx_send.at[0], dx_recv.at[0, 0], peer),
        send(look_in, look_in, dx_push.at[0], dx_got.at[0, 0], peer),
        send(bulk(2 * last), bulk(2 * last), w_send.at[0], w_recv.at[0, 0], peer),
        *[send(bulk(2 * last), bulk(2 * last), cast_send.at[e], cast_recv.at[e], peer) for e in range(share - 1)],
    ):
        copy.wait_send()


STORE_IN = pl.BlockSpec(memory_space=pl.ANY)


def _store(*refs):
    copies = [pltpu.make_async_copy(refs[i], refs[4 + i], refs[8].at[i]) for i in range(4)]
    for copy in copies:
        copy.start()
    for copy in copies:
        copy.wait()


def solution(mesh):
    tp = mesh.shape["tp"]
    n = tp // 2
    dp = mesh.shape["dp"]
    side = math.isqrt(dp)
    share = 4 if side * side == dp and side % 2 == 0 else 1

    def shard_step(token_ids, emb_table, norm_gain, w_in, w_out, d_out):
        v_rows, dim = emb_table.shape
        hid = w_out.shape[0]
        rows = d_out.shape[0]
        half = rows // 2
        lane = min(128, half)
        v_pad = -(-v_rows // 512) * 512
        vmem = pl.BlockSpec(memory_space=pltpu.VMEM)
        hbm = pl.BlockSpec(memory_space=pl.ANY)
        dma = pltpu.SemaphoreType.DMA
        results = pl.pallas_call(
            functools.partial(_kernel, n, side, share),
            out_shape=(
                pltpu.VMEM((rows, dim), BF16),
                pltpu.VMEM((v_rows, dim), F32),
                pltpu.VMEM((dim, hid), F32),
                pltpu.VMEM((hid, dim), F32),
            ),
            in_specs=[hbm] * 6,
            out_specs=(vmem,) * 4,
            scratch_shapes=[
                pltpu.VMEM((token_ids.shape[0] // lane, 1, lane), jnp.int32),
                pltpu.VMEM((dim // 128, 128), BF16),
                pltpu.VMEM((rows, dim), BF16),
                pltpu.VMEM((v_pad, dim), BF16),
                pltpu.VMEM((n, 2, half, dim), BF16),
                pltpu.VMEM((n, 2, half, dim), BF16),
                pltpu.VMEM((tp, dim, hid), BF16),
                pltpu.VMEM((tp, hid, dim), BF16),
                pltpu.VMEM((2, n - 1, half, dim), BF16),
                pltpu.VMEM((2, n - 1, half, dim), BF16),
                pltpu.VMEM((rows, dim), F32),
                pltpu.VMEM((rows, dim), BF16),
                pltpu.VMEM((dim, rows), BF16),
                pltpu.VMEM((dim, rows), BF16),
                pltpu.VMEM((n, half, 2 * hid), BF16),
                pltpu.VMEM((n, half, 2 * hid), BF16),
                pltpu.VMEM((n, half, 2 * hid), BF16),
                pltpu.VMEM((rows, dim), F32),
                pltpu.VMEM((rows, dim), F32),
                pltpu.VMEM((tp, 2, dim, hid), F32),
                pltpu.VMEM((n, 2, dim, hid), F32),
                pltpu.VMEM((2, n - 1, dim, hid), F32),
                pltpu.VMEM((tp, rows, dim), BF16),
                dma((6,)),
                dma((1,)), dma((2, n // 2)), dma((1,)), dma((1,)),
                dma((max(share - 1, 1),)), dma((max(share - 1, 1),)),
                dma((1,)), dma((2, n - 1)), dma((1,)), dma((n,)),
                dma((1,)), dma((2, n)), dma((1,)), dma((2, n - 1)),
                dma((1,)), dma((2, n - 1)), dma((1,)), dma((2, n + 1)),
            ],
            compiler_params=pltpu.CompilerParams(
                collective_id=0, has_side_effects=True, vmem_limit_bytes=57 * 1024 * 1024
            ),
            name="block_step",
        )(token_ids.reshape(-1, 1, lane), emb_table, norm_gain.reshape(-1, 128), w_in, w_out, d_out)
        return pl.pallas_call(
            _store,
            out_shape=tuple(jax.ShapeDtypeStruct(r.shape, r.dtype) for r in results),
            in_specs=[STORE_IN] * 4,
            out_specs=(hbm,) * 4,
            scratch_shapes=[dma((4,))],
            compiler_params=pltpu.CompilerParams(vmem_limit_bytes=1024 * 1024),
            name="store",
        )(*results)

    return jax.shard_map(
        shard_step,
        mesh=mesh,
        in_specs=(P("dp"), P("tp", None), P(None), P(None, "tp"), P("tp", None), P(("dp", "tp"), None)),
        out_specs=(P(("dp", "tp"), None), P(("dp", "tp"), None), P("dp", "tp"), P(("dp", "tp"), None)),
        check_vma=False,
    )
```

```python
import functools
import math

import jax
import jax.numpy as jnp
from jax import lax
from jax.experimental import pallas as pl
from jax.experimental.pallas import tpu as pltpu
from jax.sharding import PartitionSpec as P

EPS = 1e-6
F32, BF16 = jnp.float32, jnp.bfloat16
NT = (((1,), (1,)), ((), ()))


def _dot(a, b):
    return jnp.dot(a, b, preferred_element_type=F32)


def _gelu_and_grad(u):
    k0, k1 = 0.7978845608028654, 0.044715
    u2 = u * u
    t = jnp.tanh(k0 * (u + k1 * (u2 * u)))
    cdf = 0.5 * (1.0 + t)
    grad = cdf + (0.5 * u) * (1.0 - t * t) * (k0 + (3.0 * k0 * k1) * u2)
    return u * cdf, grad


def _kernel(
    n, side, share, ids_hbm, emb_ref, gain_hbm, w_in_ref, w_out_ref, d_out_hbm,
    out_ref, d_tab, d_w_in_ref, d_w_out_ref,
    ids_ref, gain_ref, d_out_ref, emb, look_out, look_in, w1, w2, first, ring, x_buf, n_buf, nt_buf, dot_buf, dh_buf, h_buf, du_buf, y_buf, dn_buf,
    dw, dw_sib, dw_ring, dx,
    load_sem, w_send, w_recv, w_push, w_got, cast_send, cast_recv, look_send, look_recv, look_push, look_got,
    dw_push, dw_got, dw_send, dw_recv, dx_send, dx_recv, dx_push, dx_got,
):
    rank = lax.axis_index("tp")
    z, c = rank // 2, rank % 2
    peer = 2 * z + (1 - c)
    far = n // 2
    last = n - 1
    hops = (2 * lax.rem(z + 1, n) + c, 2 * lax.rem(z + n - 1, n) + c)
    half, dim = first.shape[2], first.shape[3]
    v_rows, v_pad = emb_ref.shape[0], emb.shape[0]
    lane = ids_ref.shape[2]
    per_half = half // lane

    def send(src, dst, ssem, rsem, to):
        return pltpu.make_async_remote_copy(
            src_ref=src, dst_ref=dst, send_sem=ssem, recv_sem=rsem,
            device_id={"tp": to}, device_id_type=pl.DeviceIdType.MESH,
        )

    def chip(d, k):
        return lax.rem(z + (2 * d - 1) * k + 2 * n, n)

    loads = [
        pltpu.make_async_copy(src, dst, load_sem.at[i])
        for i, (src, dst) in enumerate(
            [
                (ids_hbm, ids_ref),
                (emb_ref, emb.at[pl.ds(0, v_rows)]),
                (w_in_ref, w1.at[rank]),
                (w_out_ref, w2.at[rank]),
                (d_out_hbm, d_out_ref),
                (gain_hbm, gain_ref),
            ]
        )
    ]
    for load in loads:
        load.start()
    emb[v_rows:] = jnp.zeros((v_pad - v_rows, dim), BF16)

    group = lax.axis_index("dp")
    gx, gy = group // side, group % side
    quarter = (2 * (gx % 2) + gy % 2) if share > 1 else 0
    square = []
    for e in range(1, share):
        px = gx + (e // 2) * (1 - 2 * (gx % 2))
        py = gy + (e % 2) * (1 - 2 * (gy % 2))
        square.append(px * side + py)

    barrier = pltpu.get_barrier_semaphore()
    for other in (*hops, peer):
        pl.semaphore_signal(barrier, inc=1, device_id={"tp": other}, device_id_type=pl.DeviceIdType.MESH)
    for other in square:
        pl.semaphore_signal(barrier, inc=1, device_id={"dp": other}, device_id_type=pl.DeviceIdType.MESH)
    def w_part(w, ref):
        size = ref.shape[0] // share
        return ref.at[pl.ds(pl.multiple_of(quarter * size, size), size)]

    def w_block(w, d, m):
        return (w1, w2)[w].at[2 * chip(d, m) + c]

    def w_copy(d, m, w, own=False):
        dst = w_part(w, w_block(w, d, m))
        src = w_part(w, (w_in_ref, w_out_ref)[w]) if own else dst
        return send(src, dst, w_send.at[0], w_recv.at[d, m], hops[d])

    def w_casts(d, m, w):
        part = w_part(w, w_block(w, d, m))
        return [
            pltpu.make_async_remote_copy(
                src_ref=part, dst_ref=part,
                send_sem=cast_send.at[e], recv_sem=cast_recv.at[e],
                device_id={"dp": other}, device_id_type=pl.DeviceIdType.MESH,
            )
            for e, other in enumerate(square)
        ]

    def w_peer(d, m, w, own=False):
        dst = w_block(w, d, m)
        src = (w_in_ref, w_out_ref)[w] if own else dst
        return send(src, dst, w_push.at[0], w_got.at[0], peer)

    blocks = [(d, m, w) for m in range(1, far + 1) for d in range(2) for w in range(2) if m < far or w == d]

    def bulk(parts):
        rows = parts * w2.shape[1] // share
        return dx.at[0, pl.ds(0, rows)] if rows <= dx.shape[1] else w2.at[pl.ds(0, parts)]

    def w_stage(m):
        for d in range(2):
            came = bulk(2 if m < far else 1)
            send(came, came, w_send.at[0], w_recv.at[d, m - 1], hops[d]).wait_recv()
        for d, k, w in blocks:
            if k == m:
                if m < far - 1 or (m == far - 1 and w == d):
                    w_copy(d, m, w).start()
                for copy in w_casts(d, m, w):
                    copy.start()

    def w_share():
        for e in range(share - 1):
            send(bulk(2 * last), bulk(2 * last), cast_send.at[e], cast_recv.at[e], peer).wait_recv()
        for d, m, w in blocks:
            w_peer(d, m, w).start()

    lanes = lax.broadcasted_iota(jnp.int32, (2 * half, v_pad), 1)

    def wanted(j, h, core):
        at = (2 * (2 * j + core) + h) * per_half
        return [jnp.broadcast_to(ids_ref[at + i], (lane, lane)).T for i in range(per_half)]

    def look_half(d, p):
        if isinstance(p, int) and p == 0:
            return 1 - d
        return (p + 1) % 2 + d * (p // last)

    def looked_up(p, core):
        k = far - (p + 1) // 2
        want = jnp.concatenate(
            [t for d in range(2) for t in wanted(chip(1 - d, k), look_half(d, p), core)], axis=0
        )
        want = jnp.concatenate([want - rank * v_rows] * (v_pad // lane), axis=1)
        return _dot(jnp.where(want == lanes, 1.0, 0.0).astype(BF16), emb[...])

    def look_peer(slot):
        return send(look_out.at[slot], look_in.at[slot], look_push.at[0], look_got.at[slot], peer)

    def for_peer(slot):
        part = looked_up(slot, 1 - c).astype(BF16)
        for d in range(2):
            look_out[slot, d] = part[d * half : (d + 1) * half]

    def look_copy(d, p):
        return send(first.at[d, p], ring.at[d, p], look_send.at[0], look_recv.at[d, p], hops[d])

    loads[0].wait()
    loads[1].wait()
    for_peer(0)
    pl.semaphore_wait(barrier, 2 + share)
    look_peer(0).start()
    for d in range(2):
        for w in range(2):
            w_copy(d, 0, w, True).start()
    for w in range(2):
        w_peer(0, 0, w, True).start()
    x_buf[...] = looked_up(0, c)
    look_peer(0).wait_recv()
    for d in range(2):
        first[d, 0] = (x_buf[pl.ds(d * half, half)] + look_in[0, d].astype(F32)).astype(BF16)
        look_copy(d, 0).start()
    for_peer(1)
    look_peer(1).start()
    for load in loads[2:]:
        load.wait()

    def gather_round(p, carry):
        x_buf[...] = looked_up(p, c)
        for m in range(1, far + 1):

            @pl.when(p == m)
            def _():
                w_stage(m)

        look_peer(p).wait_recv()
        for d in range(2):
            first[d, p] = (x_buf[pl.ds(d * half, half)] + look_in[p, d].astype(F32)).astype(BF16)

            @pl.when(p > 2 if d else p >= 2)
            def _():
                look_copy(d, p - 2).wait_recv()
                first[d, p] = (first[d, p].astype(F32) + ring[d, p - 2].astype(F32)).astype(BF16)

            if d:

                @pl.when(p == 1)
                def _():
                    look_copy(d, 0).wait_recv()
                    first[d, p] = (first[d, p].astype(F32) + ring[d, 0].astype(F32)).astype(BF16)

            look_copy(d, p).start()

        @pl.when(p == far + 1)
        def _():
            w_share()

        for_peer(p + 1)
        look_peer(p + 1).start()
        return carry

    lax.fori_loop(1, last, gather_round, 0)
    x_buf[...] = looked_up(last, c)
    look_peer(last).wait_recv()
    x_buf[...] = x_buf[...] + jnp.concatenate([look_in[last, h] for h in range(2)], axis=0).astype(F32)
    dot_buf[...] = d_out_ref[...].astype(F32).T.astype(BF16)
    y_buf[...] = jnp.zeros_like(y_buf)
    dn_buf[...] = jnp.zeros_like(dn_buf)
    gain = jnp.concatenate([gain_ref[i : i + 1].astype(F32) for i in range(gain_ref.shape[0])], axis=1)

    def norm(h):
        p = last - 2 + h
        at = pl.ds(h * half, half)
        for d in range(2):
            look_copy(d, p).wait_recv()
        x = x_buf[at] + (ring[0, p].astype(F32) + ring[1, p].astype(F32))
        x_buf[at] = x
        normed = (x * lax.rsqrt(jnp.mean(x * x, axis=-1, keepdims=True) + EPS) * gain).astype(BF16)
        n_buf[at] = normed
        nt_buf[:, pl.ds(h * half, half)] = normed.astype(F32).T.astype(BF16)

    def dw_peer(d, j):
        return send(dw.at[2 * j + (1 - c), d], dw_sib.at[j, d], dw_push.at[0], dw_got.at[d, j], peer)

    def dw_where(d, p):
        return chip(1 - d, far - (p + 1) // 2), d + (1 - 2 * d) * (p % 2)

    def dw_copy(d, p):
        j, h = dw_where(d, p)
        return send(dw.at[2 * j + c, h], dw_ring.at[d, p], dw_send.at[0], dw_recv.at[d, p], hops[d])

    def dw_step(p, fresh=False, ways=(0, 1)):
        for d in ways:
            j, h = dw_where(d, p)
            dw_peer(h, j).wait_recv()
            if fresh:
                dw[2 * j + c, h] = dw[2 * j + c, h] + dw_sib[j, h]
            else:
                dw_copy(d, p - 2).wait_recv()
                dw[2 * j + c, h] = (dw[2 * j + c, h] + dw_sib[j, h]) + dw_ring[d, p - 2]
            dw_copy(d, p).start()

    def tile_chip(i):
        return chip(i % 2, far - (i + 1) // 2)

    send(w1, w1, w_push.at[0], w_got.at[0], peer).wait_recv()

    def weights(i):
        j = tile_chip(i)
        w1t = jnp.concatenate([w1[2 * j], w1[2 * j + 1]], axis=1)
        w2t = jnp.concatenate([w2[2 * j], w2[2 * j + 1]], axis=0)
        return j, w1t, w2t

    def hidden_grad(i, h):
        out_grad = d_out_ref[pl.ds(h * half, half)]
        return lax.dot_general(out_grad, weights(i)[2], NT, preferred_element_type=F32).astype(BF16)

    def early(i, carry):
        for t in (2 * i, 2 * i + 1):
            dh_buf[t] = hidden_grad(t, 0)
        return carry

    def inner(i, h, d_h):
        at = pl.ds(h * half, half)
        w1t = weights(i)[1]
        act, grad = _gelu_and_grad(_dot(n_buf[at], w1t).astype(BF16).astype(F32))
        hidden = act.astype(BF16)
        d_u = (d_h.astype(F32) * grad).astype(BF16)
        return hidden, d_u, lax.dot_general(d_u, w1t, NT, preferred_element_type=F32)

    def first_half(i, carry):
        total = dn_buf[:half]
        for t in (2 * i, 2 * i + 1):
            h_buf[t], du_buf[t], more = inner(t, 0, dh_buf[t])
            total = total + more
        dn_buf[:half] = total
        return carry

    def second_half(i, carry):
        j, _, w2t = weights(i)
        hid = w1.shape[2]
        hidden, d_u, more = inner(i, 1, hidden_grad(i, 1))
        dn_buf[half:] += more
        hidden = jnp.concatenate([h_buf[i], hidden], axis=0)
        d_u = jnp.concatenate([du_buf[i], d_u], axis=0)
        for which, g in ((0, _dot(nt_buf[...], d_u)), (1, _dot(dot_buf[...], hidden))):
            for q in range(2):
                dw[2 * j + q, which] = g[:, q * hid : (q + 1) * hid]
        for d in range(2):
            dw_peer(d, j).start()
        y_buf[...] += _dot(hidden, w2t)

        for at, p in ((1, 0), (3, 1)):

            @pl.when(i == at)
            def _():
                dw_step(p, fresh=True)

        return carry

    def leave(h):
        at = pl.ds(h * half, half)
        x = x_buf[at]
        d_scaled = dn_buf[at] * gain
        inv_rms = lax.rsqrt(jnp.mean(x * x, axis=-1, keepdims=True) + EPS)
        row_proj = jnp.mean(d_scaled * x, axis=-1, keepdims=True)
        dx[rank, at] = (
            d_out_ref[at].astype(F32) + inv_rms * (d_scaled - x * inv_rms * inv_rms * row_proj)
        ).astype(BF16)
        for d in range(2):
            dx_copy(d, h).start()
        dx_peer(h, h).start()

    def dx_where(d, p):
        return chip(d, p // 2), p % 2 + d * (p // n)

    def dx_piece(d, p, core):
        j, h = dx_where(d, p)
        return dx.at[2 * j + core, pl.ds(pl.multiple_of(h * half, half), half)]

    def dx_copy(d, p):
        piece = dx_piece(d, p + d * (p // (last - 1)), c)
        return send(piece, piece, dx_send.at[0], dx_recv.at[d, p], hops[d])

    def dx_peer(d, p):
        piece = dx_piece(d, p, c)
        return send(piece, piece, dx_push.at[0], dx_got.at[d, p], peer)

    v_tile = v_pad // 4

    def add_rows(pieces, fresh=False):
        def tile(v, carry, size=v_tile):
            at = pl.ds(v * v_tile if isinstance(v, int) else pl.multiple_of(v * v_tile, v_tile), size)
            rows = lax.broadcasted_iota(jnp.int32, (size, half), 0)
            total = None if fresh else d_tab[at]
            for d, p, core in pieces:
                j, h = dx_where(d, p)
                i0 = (2 * (2 * j + core) + h) * per_half
                ids = jnp.concatenate([ids_ref[i0 + i] for i in range(per_half)], axis=1)
                place = jnp.where(rows == ids - (rank * v_rows + v * v_tile), 1.0, 0.0).astype(BF16)
                more = _dot(place, dx[2 * j + core, pl.ds(pl.multiple_of(h * half, half), half)])
                total = more if total is None else total + more
            d_tab[at] = total
            return carry

        lax.fori_loop(0, v_rows // v_tile, tile, 0)
        if v_rows % v_tile:
            tile(v_rows // v_tile, 0, v_rows % v_tile)

    lax.fori_loop(0, n // 2, early, 0)
    norm(0)
    lax.fori_loop(0, n // 2, first_half, 0)
    leave(0)
    norm(1)
    lax.fori_loop(0, n, second_half, 0)
    leave(1)
    out_ref[...] = (x_buf[...] + y_buf[...]).astype(BF16)
    dw_step(2)
    add_rows([(0, 0, c), (0, 1, c)], fresh=True)

    def scatter_round(p, carry):
        for d in range(2):
            dx_copy(d, p - 2).wait_recv()
            dx_copy(d, p).start()
            dx_peer(d, p).start()

        @pl.when(p == 2)
        def _():
            for d in range(2):
                dx_peer(d, d).wait_recv()

        @pl.when(p > 2)
        def _():
            for d in range(2):
                dx_peer(d, p - 1).wait_recv()

        add_rows([(0, p, c), (1, p, c), (0, (p - 1) * ((p + 1) // 4), 1 - c), (1, p - 1, 1 - c)])

        @pl.when(p > 2)
        def _():
            dw_step(p)

        return carry

    lax.fori_loop(2, last - 1, scatter_round, 0)

    def finish(p, ways):
        for d in range(2):
            dx_peer(d, p - 1).wait_recv()
        add_rows([(0, p - 1, 1 - c), (1, p - 1, 1 - c)])
        for d in range(2):
            dx_copy(d, p - 2).wait_recv()
            if d in ways:
                dx_copy(d, last - 1).start()
            dx_peer(d, p).start()
        add_rows([(0, p, c), (1, p, c)])
        if ways:
            dw_step(last - 1, ways=ways)

    finish(last - 1, (0,))
    finish(last, (1,))
    finish(last + 1, ())
    for d in range(2):
        dx_peer(d, last + 1).wait_recv()
    add_rows([(0, last + 1, 1 - c), (1, last + 1, 1 - c)])
    sums = []
    for h in range(2):
        dw_peer(h, z).wait_recv()
        sums.append(dw[rank, h] + dw_sib[z, h])
    for d in range(2):
        dw_copy(d, last - 2).wait_recv()
    for d in range(2):
        dw_copy(d, last - 1).wait_recv()
    d_w_in_ref[...] = (sums[0] + dw_ring[1, last - 2]) + dw_ring[0, last - 1]
    d_w_out_ref[...] = ((sums[1] + dw_ring[0, last - 2]) + dw_ring[1, last - 1]).T

    for copy in (
        send(first, ring, look_send.at[0], look_recv.at[0, 0], peer),
        send(look_out, look_in, look_push.at[0], look_got.at[0], peer),
        send(w1, w1, w_push.at[0], w_got.at[0], peer),
        send(dw_sib, dw_sib, dw_push.at[0], dw_got.at[0, 0], peer),
        send(dw_ring, dw_ring, dw_send.at[0], dw_recv.at[0, 0], peer),
        send(ring, ring, dx_send.at[0], dx_recv.at[0, 0], peer),
        send(look_in, look_in, dx_push.at[0], dx_got.at[0, 0], peer),
        send(bulk(2 * last), bulk(2 * last), w_send.at[0], w_recv.at[0, 0], peer),
        *[send(bulk(2 * last), bulk(2 * last), cast_send.at[e], cast_recv.at[e], peer) for e in range(share - 1)],
    ):
        copy.wait_send()


STORE_IN = pl.BlockSpec(memory_space=pl.ANY)


def _store(*refs):
    copies = [pltpu.make_async_copy(refs[i], refs[4 + i], refs[8].at[i]) for i in range(4)]
    for copy in copies:
        copy.start()
    for copy in copies:
        copy.wait()


def solution(mesh):
    tp = mesh.shape["tp"]
    n = tp // 2
    dp = mesh.shape["dp"]
    side = math.isqrt(dp)
    share = 4 if side * side == dp and side % 2 == 0 else 1

    def shard_step(token_ids, emb_table, norm_gain, w_in, w_out, d_out):
        v_rows, dim = emb_table.shape
        hid = w_out.shape[0]
        rows = d_out.shape[0]
        half = rows // 2
        lane = min(128, half)
        v_pad = -(-v_rows // 512) * 512
        vmem = pl.BlockSpec(memory_space=pltpu.VMEM)
        hbm = pl.BlockSpec(memory_space=pl.ANY)
        dma = pltpu.SemaphoreType.DMA
        results = pl.pallas_call(
            functools.partial(_kernel, n, side, share),
            out_shape=(
                pltpu.VMEM((rows, dim), BF16),
                pltpu.VMEM((v_rows, dim), F32),
                pltpu.VMEM((dim, hid), F32),
                pltpu.VMEM((hid, dim), F32),
            ),
            in_specs=[hbm] * 6,
            out_specs=(vmem,) * 4,
            scratch_shapes=[
                pltpu.VMEM((token_ids.shape[0] // lane, 1, lane), jnp.int32),
                pltpu.VMEM((dim // 128, 128), BF16),
                pltpu.VMEM((rows, dim), BF16),
                pltpu.VMEM((v_pad, dim), BF16),
                pltpu.VMEM((n, 2, half, dim), BF16),
                pltpu.VMEM((n, 2, half, dim), BF16),
                pltpu.VMEM((tp, dim, hid), BF16),
                pltpu.VMEM((tp, hid, dim), BF16),
                pltpu.VMEM((2, n - 1, half, dim), BF16),
                pltpu.VMEM((2, n - 1, half, dim), BF16),
                pltpu.VMEM((rows, dim), F32),
                pltpu.VMEM((rows, dim), BF16),
                pltpu.VMEM((dim, rows), BF16),
                pltpu.VMEM((dim, rows), BF16),
                pltpu.VMEM((n, half, 2 * hid), BF16),
                pltpu.VMEM((n, half, 2 * hid), BF16),
                pltpu.VMEM((n, half, 2 * hid), BF16),
                pltpu.VMEM((rows, dim), F32),
                pltpu.VMEM((rows, dim), F32),
                pltpu.VMEM((tp, 2, dim, hid), F32),
                pltpu.VMEM((n, 2, dim, hid), F32),
                pltpu.VMEM((2, n - 1, dim, hid), F32),
                pltpu.VMEM((tp, rows, dim), BF16),
                dma((6,)),
                dma((1,)), dma((2, n // 2)), dma((1,)), dma((1,)),
                dma((max(share - 1, 1),)), dma((max(share - 1, 1),)),
                dma((1,)), dma((2, n - 1)), dma((1,)), dma((n,)),
                dma((1,)), dma((2, n)), dma((1,)), dma((2, n - 1)),
                dma((1,)), dma((2, n - 1)), dma((1,)), dma((2, n + 1)),
            ],
            compiler_params=pltpu.CompilerParams(
                collective_id=0, has_side_effects=True, vmem_limit_bytes=57 * 1024 * 1024
            ),
            name="block_step",
        )(token_ids.reshape(-1, 1, lane), emb_table, norm_gain.reshape(-1, 128), w_in, w_out, d_out)
        return pl.pallas_call(
            _store,
            out_shape=tuple(jax.ShapeDtypeStruct(r.shape, r.dtype) for r in results),
            in_specs=[STORE_IN] * 4,
            out_specs=(hbm,) * 4,
            scratch_shapes=[dma((4,))],
            compiler_params=pltpu.CompilerParams(vmem_limit_bytes=1024 * 1024),
            name="store",
        )(*results)

    return jax.shard_map(
        shard_step,
        mesh=mesh,
        in_specs=(P("dp"), P("tp", None), P(None), P(None, "tp"), P("tp", None), P(("dp", "tp"), None)),
        out_specs=(P(("dp", "tp"), None), P(("dp", "tp"), None), P("dp", "tp"), P(("dp", "tp"), None)),
        check_vma=False,
    )
```

```python
import functools
import math

import jax
import jax.numpy as jnp
from jax import lax
from jax.experimental import pallas as pl
from jax.experimental.pallas import tpu as pltpu
from jax.sharding import PartitionSpec as P

EPS = 1e-6
F32, BF16 = jnp.float32, jnp.bfloat16
NT = (((1,), (1,)), ((), ()))


def _dot(a, b):
    return jnp.dot(a, b, preferred_element_type=F32)


def _gelu_and_grad(u):
    k0, k1 = 0.7978845608028654, 0.044715
    u2 = u * u
    t = jnp.tanh(k0 * (u + k1 * (u2 * u)))
    cdf = 0.5 * (1.0 + t)
    grad = cdf + (0.5 * u) * (1.0 - t * t) * (k0 + (3.0 * k0 * k1) * u2)
    return u * cdf, grad


def _kernel(
    n, side, share, ids_hbm, emb_ref, gain_hbm, w_in_ref, w_out_ref, d_out_hbm,
    out_ref, d_tab, d_w_in_ref, d_w_out_ref,
    ids_ref, gain_ref, d_out_ref, emb, look_out, look_in, w1, w2, first, ring, x_buf, n_buf, nt_buf, dot_buf, dh_buf, h_buf, du_buf, y_buf, dn_buf,
    dw, dw_sib, dw_ring, dx,
    load_sem, w_send, w_recv, w_push, w_got, cast_send, cast_recv, look_send, look_recv, look_push, look_got,
    dw_push, dw_got, dw_send, dw_recv, dx_send, dx_recv, dx_push, dx_got,
):
    rank = lax.axis_index("tp")
    z, c = rank // 2, rank % 2
    peer = 2 * z + (1 - c)
    far = n // 2
    last = n - 1
    hops = (2 * lax.rem(z + 1, n) + c, 2 * lax.rem(z + n - 1, n) + c)
    half, dim = first.shape[2], first.shape[3]
    v_rows, v_pad = emb_ref.shape[0], emb.shape[0]
    lane = ids_ref.shape[2]
    per_half = half // lane

    def send(src, dst, ssem, rsem, to):
        return pltpu.make_async_remote_copy(
            src_ref=src, dst_ref=dst, send_sem=ssem, recv_sem=rsem,
            device_id={"tp": to}, device_id_type=pl.DeviceIdType.MESH,
        )

    def chip(d, k):
        return lax.rem(z + (2 * d - 1) * k + 2 * n, n)

    loads = [
        pltpu.make_async_copy(src, dst, load_sem.at[i])
        for i, (src, dst) in enumerate(
            [
                (ids_hbm, ids_ref),
                (emb_ref, emb.at[pl.ds(0, v_rows)]),
                (w_in_ref, w1.at[rank]),
                (w_out_ref, w2.at[rank]),
                (d_out_hbm, d_out_ref),
                (gain_hbm, gain_ref),
            ]
        )
    ]
    for load in loads:
        load.start()
    emb[v_rows:] = jnp.zeros((v_pad - v_rows, dim), BF16)

    group = lax.axis_index("dp")
    gx, gy = group // side, group % side
    quarter = (2 * (gx % 2) + gy % 2) if share > 1 else 0
    square = []
    for e in range(1, share):
        px = gx + (e // 2) * (1 - 2 * (gx % 2))
        py = gy + (e % 2) * (1 - 2 * (gy % 2))
        square.append(px * side + py)

    barrier = pltpu.get_barrier_semaphore()
    for other in (*hops, peer):
        pl.semaphore_signal(barrier, inc=1, device_id={"tp": other}, device_id_type=pl.DeviceIdType.MESH)
    for other in square:
        pl.semaphore_signal(barrier, inc=1, device_id={"dp": other}, device_id_type=pl.DeviceIdType.MESH)
    def w_part(w, ref):
        size = ref.shape[0] // share
        return ref.at[pl.ds(pl.multiple_of(quarter * size, size), size)]

    def w_block(w, d, m):
        return (w1, w2)[w].at[2 * chip(d, m) + c]

    def w_copy(d, m, w, own=False):
        dst = w_part(w, w_block(w, d, m))
        src = w_part(w, (w_in_ref, w_out_ref)[w]) if own else dst
        return send(src, dst, w_send.at[0], w_recv.at[d, m], hops[d])

    def w_casts(d, m, w):
        part = w_part(w, w_block(w, d, m))
        return [
            pltpu.make_async_remote_copy(
                src_ref=part, dst_ref=part,
                send_sem=cast_send.at[e], recv_sem=cast_recv.at[e],
                device_id={"dp": other}, device_id_type=pl.DeviceIdType.MESH,
            )
            for e, other in enumerate(square)
        ]

    def w_peer(d, m, w, own=False):
        dst = w_block(w, d, m)
        src = (w_in_ref, w_out_ref)[w] if own else dst
        return send(src, dst, w_push.at[0], w_got.at[0], peer)

    blocks = [(d, m, w) for m in range(1, far + 1) for d in range(2) for w in range(2) if m < far or w == d]

    def bulk(parts):
        rows = parts * w2.shape[1] // share
        return dx.at[0, pl.ds(0, rows)] if rows <= dx.shape[1] else w2.at[pl.ds(0, parts)]

    def w_stage(m):
        for d in range(2):
            came = bulk(2 if m < far else 1)
            send(came, came, w_send.at[0], w_recv.at[d, m - 1], hops[d]).wait_recv()
        for d, k, w in blocks:
            if k == m:
                if m < far - 1 or (m == far - 1 and w == d):
                    w_copy(d, m, w).start()
                for copy in w_casts(d, m, w):
                    copy.start()

    def w_share():
        for e in range(share - 1):
            send(bulk(2 * last), bulk(2 * last), cast_send.at[e], cast_recv.at[e], peer).wait_recv()
        for d, m, w in blocks:
            w_peer(d, m, w).start()

    lanes = lax.broadcasted_iota(jnp.int32, (2 * half, v_pad), 1)

    def wanted(j, h, core):
        at = (2 * (2 * j + core) + h) * per_half
        return [jnp.broadcast_to(ids_ref[at + i], (lane, lane)).T for i in range(per_half)]

    def look_half(d, p):
        if isinstance(p, int) and p == 0:
            return 1 - d
        return (p + 1) % 2 + d * (p // last)

    def looked_up(p, core):
        k = far - (p + 1) // 2
        want = jnp.concatenate(
            [t for d in range(2) for t in wanted(chip(1 - d, k), look_half(d, p), core)], axis=0
        )
        want = jnp.concatenate([want - rank * v_rows] * (v_pad // lane), axis=1)
        return _dot(jnp.where(want == lanes, 1.0, 0.0).astype(BF16), emb[...])

    def look_peer(slot):
        return send(look_out.at[slot], look_in.at[slot], look_push.at[0], look_got.at[slot], peer)

    def for_peer(slot):
        part = looked_up(slot, 1 - c).astype(BF16)
        for d in range(2):
            look_out[slot, d] = part[d * half : (d + 1) * half]

    def look_copy(d, p):
        return send(first.at[d, p], ring.at[d, p], look_send.at[0], look_recv.at[d, p], hops[d])

    loads[0].wait()
    loads[1].wait()
    for_peer(0)
    pl.semaphore_wait(barrier, 2 + share)
    look_peer(0).start()
    for d in range(2):
        for w in range(2):
            w_copy(d, 0, w, True).start()
    for w in range(2):
        w_peer(0, 0, w, True).start()
    x_buf[...] = looked_up(0, c)
    look_peer(0).wait_recv()
    for d in range(2):
        first[d, 0] = (x_buf[pl.ds(d * half, half)] + look_in[0, d].astype(F32)).astype(BF16)
        look_copy(d, 0).start()
    for_peer(1)
    look_peer(1).start()
    for load in loads[2:]:
        load.wait()

    def gather_round(p, carry):
        x_buf[...] = looked_up(p, c)
        for m in range(1, far + 1):

            @pl.when(p == m)
            def _():
                w_stage(m)

        look_peer(p).wait_recv()
        for d in range(2):
            first[d, p] = (x_buf[pl.ds(d * half, half)] + look_in[p, d].astype(F32)).astype(BF16)

            @pl.when(p > 2 if d else p >= 2)
            def _():
                look_copy(d, p - 2).wait_recv()
                first[d, p] = (first[d, p].astype(F32) + ring[d, p - 2].astype(F32)).astype(BF16)

            if d:

                @pl.when(p == 1)
                def _():
                    look_copy(d, 0).wait_recv()
                    first[d, p] = (first[d, p].astype(F32) + ring[d, 0].astype(F32)).astype(BF16)

            look_copy(d, p).start()

        @pl.when(p == far + 1)
        def _():
            w_share()

        for_peer(p + 1)
        look_peer(p + 1).start()
        return carry

    lax.fori_loop(1, last, gather_round, 0)
    x_buf[...] = looked_up(last, c)
    look_peer(last).wait_recv()
    x_buf[...] = x_buf[...] + jnp.concatenate([look_in[last, h] for h in range(2)], axis=0).astype(F32)
    dot_buf[...] = d_out_ref[...].astype(F32).T.astype(BF16)
    y_buf[...] = jnp.zeros_like(y_buf)
    dn_buf[...] = jnp.zeros_like(dn_buf)
    gain = jnp.concatenate([gain_ref[i : i + 1].astype(F32) for i in range(gain_ref.shape[0])], axis=1)

    def norm(h):
        p = last - 2 + h
        at = pl.ds(h * half, half)
        for d in range(2):
            look_copy(d, p).wait_recv()
        x = x_buf[at] + (ring[0, p].astype(F32) + ring[1, p].astype(F32))
        x_buf[at] = x
        normed = (x * lax.rsqrt(jnp.mean(x * x, axis=-1, keepdims=True) + EPS) * gain).astype(BF16)
        n_buf[at] = normed
        nt_buf[:, pl.ds(h * half, half)] = normed.astype(F32).T.astype(BF16)

    def dw_peer(d, j):
        return send(dw.at[2 * j + (1 - c), d], dw_sib.at[j, d], dw_push.at[0], dw_got.at[d, j], peer)

    def dw_where(d, p):
        return chip(1 - d, far - (p + 1) // 2), d + (1 - 2 * d) * (p % 2)

    def dw_copy(d, p):
        j, h = dw_where(d, p)
        return send(dw.at[2 * j + c, h], dw_ring.at[d, p], dw_send.at[0], dw_recv.at[d, p], hops[d])

    def dw_step(p, fresh=False, ways=(0, 1)):
        for d in ways:
            j, h = dw_where(d, p)
            dw_peer(h, j).wait_recv()
            if fresh:
                dw[2 * j + c, h] = dw[2 * j + c, h] + dw_sib[j, h]
            else:
                dw_copy(d, p - 2).wait_recv()
                dw[2 * j + c, h] = (dw[2 * j + c, h] + dw_sib[j, h]) + dw_ring[d, p - 2]
            dw_copy(d, p).start()

    def tile_chip(i):
        return chip(i % 2, far - (i + 1) // 2)

    send(w1, w1, w_push.at[0], w_got.at[0], peer).wait_recv()

    def weights(i):
        j = tile_chip(i)
        w1t = jnp.concatenate([w1[2 * j], w1[2 * j + 1]], axis=1)
        w2t = jnp.concatenate([w2[2 * j], w2[2 * j + 1]], axis=0)
        return j, w1t, w2t

    def hidden_grad(i, h):
        out_grad = d_out_ref[pl.ds(h * half, half)]
        return lax.dot_general(out_grad, weights(i)[2], NT, preferred_element_type=F32).astype(BF16)

    def early(i, carry):
        for t in (2 * i, 2 * i + 1):
            dh_buf[t] = hidden_grad(t, 0)
        return carry

    def inner(i, h, d_h):
        at = pl.ds(h * half, half)
        w1t = weights(i)[1]
        act, grad = _gelu_and_grad(_dot(n_buf[at], w1t).astype(BF16).astype(F32))
        hidden = act.astype(BF16)
        d_u = (d_h.astype(F32) * grad).astype(BF16)
        return hidden, d_u, lax.dot_general(d_u, w1t, NT, preferred_element_type=F32)

    def first_half(i, carry):
        total = dn_buf[:half]
        for t in (4 * i, 4 * i + 1, 4 * i + 2, 4 * i + 3):
            h_buf[t], du_buf[t], more = inner(t, 0, dh_buf[t])
            total = total + more
        dn_buf[:half] = total
        return carry

    def second_half(i, carry):
        j, _, w2t = weights(i)
        hid = w1.shape[2]
        hidden, d_u, more = inner(i, 1, hidden_grad(i, 1))
        dn_buf[half:] += more
        hidden = jnp.concatenate([h_buf[i], hidden], axis=0)
        d_u = jnp.concatenate([du_buf[i], d_u], axis=0)
        for which, g in ((0, _dot(nt_buf[...], d_u)), (1, _dot(dot_buf[...], hidden))):
            for q in range(2):
                dw[2 * j + q, which] = g[:, q * hid : (q + 1) * hid]
        for d in range(2):
            dw_peer(d, j).start()
        y_buf[...] += _dot(hidden, w2t)

        for at, p in ((1, 0), (3, 1)):

            @pl.when(i == at)
            def _():
                dw_step(p, fresh=True)

        return carry

    def leave(h):
        at = pl.ds(h * half, half)
        x = x_buf[at]
        d_scaled = dn_buf[at] * gain
        inv_rms = lax.rsqrt(jnp.mean(x * x, axis=-1, keepdims=True) + EPS)
        row_proj = jnp.mean(d_scaled * x, axis=-1, keepdims=True)
        dx[rank, at] = (
            d_out_ref[at].astype(F32) + inv_rms * (d_scaled - x * inv_rms * inv_rms * row_proj)
        ).astype(BF16)
        for d in range(2):
            dx_copy(d, h).start()
        dx_peer(h, h).start()

    def dx_where(d, p):
        return chip(d, p // 2), p % 2 + d * (p // n)

    def dx_piece(d, p, core):
        j, h = dx_where(d, p)
        return dx.at[2 * j + core, pl.ds(pl.multiple_of(h * half, half), half)]

    def dx_copy(d, p):
        piece = dx_piece(d, p + d * (p // (last - 1)), c)
        return send(piece, piece, dx_send.at[0], dx_recv.at[d, p], hops[d])

    def dx_peer(d, p):
        piece = dx_piece(d, p, c)
        return send(piece, piece, dx_push.at[0], dx_got.at[d, p], peer)

    v_tile = v_pad // 4

    def add_rows(pieces, fresh=False):
        def tile(v, carry, size=v_tile):
            at = pl.ds(v * v_tile if isinstance(v, int) else pl.multiple_of(v * v_tile, v_tile), size)
            rows = lax.broadcasted_iota(jnp.int32, (size, half), 0)
            total = None if fresh else d_tab[at]
            for d, p, core in pieces:
                j, h = dx_where(d, p)
                i0 = (2 * (2 * j + core) + h) * per_half
                ids = jnp.concatenate([ids_ref[i0 + i] for i in range(per_half)], axis=1)
                place = jnp.where(rows == ids - (rank * v_rows + v * v_tile), 1.0, 0.0).astype(BF16)
                more = _dot(place, dx[2 * j + core, pl.ds(pl.multiple_of(h * half, half), half)])
                total = more if total is None else total + more
            d_tab[at] = total
            return carry

        lax.fori_loop(0, v_rows // v_tile, tile, 0)
        if v_rows % v_tile:
            tile(v_rows // v_tile, 0, v_rows % v_tile)

    lax.fori_loop(0, n // 2, early, 0)
    norm(0)
    lax.fori_loop(0, n // 4, first_half, 0)
    leave(0)
    norm(1)
    lax.fori_loop(0, n, second_half, 0)
    leave(1)
    out_ref[...] = (x_buf[...] + y_buf[...]).astype(BF16)
    dw_step(2)
    add_rows([(0, 0, c), (0, 1, c)], fresh=True)

    def scatter_round(p, carry):
        for d in range(2):
            dx_copy(d, p - 2).wait_recv()
            dx_copy(d, p).start()
            dx_peer(d, p).start()

        @pl.when(p == 2)
        def _():
            for d in range(2):
                dx_peer(d, d).wait_recv()

        @pl.when(p > 2)
        def _():
            for d in range(2):
                dx_peer(d, p - 1).wait_recv()

        add_rows([(0, p, c), (1, p, c), (0, (p - 1) * ((p + 1) // 4), 1 - c), (1, p - 1, 1 - c)])

        @pl.when(p > 2)
        def _():
            dw_step(p)

        return carry

    lax.fori_loop(2, last - 1, scatter_round, 0)

    def finish(p, ways):
        for d in range(2):
            dx_peer(d, p - 1).wait_recv()
        add_rows([(0, p - 1, 1 - c), (1, p - 1, 1 - c)])
        for d in range(2):
            dx_copy(d, p - 2).wait_recv()
            if d in ways:
                dx_copy(d, last - 1).start()
            dx_peer(d, p).start()
        add_rows([(0, p, c), (1, p, c)])
        if ways:
            dw_step(last - 1, ways=ways)

    finish(last - 1, (0,))
    finish(last, (1,))
    finish(last + 1, ())
    for d in range(2):
        dx_peer(d, last + 1).wait_recv()
    add_rows([(0, last + 1, 1 - c), (1, last + 1, 1 - c)])
    sums = []
    for h in range(2):
        dw_peer(h, z).wait_recv()
        sums.append(dw[rank, h] + dw_sib[z, h])
    for d in range(2):
        dw_copy(d, last - 2).wait_recv()
    for d in range(2):
        dw_copy(d, last - 1).wait_recv()
    d_w_in_ref[...] = (sums[0] + dw_ring[1, last - 2]) + dw_ring[0, last - 1]
    d_w_out_ref[...] = ((sums[1] + dw_ring[0, last - 2]) + dw_ring[1, last - 1]).T

    for copy in (
        send(first, ring, look_send.at[0], look_recv.at[0, 0], peer),
        send(look_out, look_in, look_push.at[0], look_got.at[0], peer),
        send(w1, w1, w_push.at[0], w_got.at[0], peer),
        send(dw_sib, dw_sib, dw_push.at[0], dw_got.at[0, 0], peer),
        send(dw_ring, dw_ring, dw_send.at[0], dw_recv.at[0, 0], peer),
        send(ring, ring, dx_send.at[0], dx_recv.at[0, 0], peer),
        send(look_in, look_in, dx_push.at[0], dx_got.at[0, 0], peer),
        send(bulk(2 * last), bulk(2 * last), w_send.at[0], w_recv.at[0, 0], peer),
        *[send(bulk(2 * last), bulk(2 * last), cast_send.at[e], cast_recv.at[e], peer) for e in range(share - 1)],
    ):
        copy.wait_send()


STORE_IN = pl.BlockSpec(memory_space=pl.ANY)


def _store(*refs):
    copies = [pltpu.make_async_copy(refs[i], refs[4 + i], refs[8].at[i]) for i in range(4)]
    for copy in copies:
        copy.start()
    for copy in copies:
        copy.wait()


def solution(mesh):
    tp = mesh.shape["tp"]
    n = tp // 2
    dp = mesh.shape["dp"]
    side = math.isqrt(dp)
    share = 4 if side * side == dp and side % 2 == 0 else 1

    def shard_step(token_ids, emb_table, norm_gain, w_in, w_out, d_out):
        v_rows, dim = emb_table.shape
        hid = w_out.shape[0]
        rows = d_out.shape[0]
        half = rows // 2
        lane = min(128, half)
        v_pad = -(-v_rows // 512) * 512
        vmem = pl.BlockSpec(memory_space=pltpu.VMEM)
        hbm = pl.BlockSpec(memory_space=pl.ANY)
        dma = pltpu.SemaphoreType.DMA
        results = pl.pallas_call(
            functools.partial(_kernel, n, side, share),
            out_shape=(
                pltpu.VMEM((rows, dim), BF16),
                pltpu.VMEM((v_rows, dim), F32),
                pltpu.VMEM((dim, hid), F32),
                pltpu.VMEM((hid, dim), F32),
            ),
            in_specs=[hbm] * 6,
            out_specs=(vmem,) * 4,
            scratch_shapes=[
                pltpu.VMEM((token_ids.shape[0] // lane, 1, lane), jnp.int32),
                pltpu.VMEM((dim // 128, 128), BF16),
                pltpu.VMEM((rows, dim), BF16),
                pltpu.VMEM((v_pad, dim), BF16),
                pltpu.VMEM((n, 2, half, dim), BF16),
                pltpu.VMEM((n, 2, half, dim), BF16),
                pltpu.VMEM((tp, dim, hid), BF16),
                pltpu.VMEM((tp, hid, dim), BF16),
                pltpu.VMEM((2, n - 1, half, dim), BF16),
                pltpu.VMEM((2, n - 1, half, dim), BF16),
                pltpu.VMEM((rows, dim), F32),
                pltpu.VMEM((rows, dim), BF16),
                pltpu.VMEM((dim, rows), BF16),
                pltpu.VMEM((dim, rows), BF16),
                pltpu.VMEM((n, half, 2 * hid), BF16),
                pltpu.VMEM((n, half, 2 * hid), BF16),
                pltpu.VMEM((n, half, 2 * hid), BF16),
                pltpu.VMEM((rows, dim), F32),
                pltpu.VMEM((rows, dim), F32),
                pltpu.VMEM((tp, 2, dim, hid), F32),
                pltpu.VMEM((n, 2, dim, hid), F32),
                pltpu.VMEM((2, n - 1, dim, hid), F32),
                pltpu.VMEM((tp, rows, dim), BF16),
                dma((6,)),
                dma((1,)), dma((2, n // 2)), dma((1,)), dma((1,)),
                dma((max(share - 1, 1),)), dma((max(share - 1, 1),)),
                dma((1,)), dma((2, n - 1)), dma((1,)), dma((n,)),
                dma((1,)), dma((2, n)), dma((1,)), dma((2, n - 1)),
                dma((1,)), dma((2, n - 1)), dma((1,)), dma((2, n + 1)),
            ],
            compiler_params=pltpu.CompilerParams(
                collective_id=0, has_side_effects=True, vmem_limit_bytes=57 * 1024 * 1024
            ),
            name="block_step",
        )(token_ids.reshape(-1, 1, lane), emb_table, norm_gain.reshape(-1, 128), w_in, w_out, d_out)
        return pl.pallas_call(
            _store,
            out_shape=tuple(jax.ShapeDtypeStruct(r.shape, r.dtype) for r in results),
            in_specs=[STORE_IN] * 4,
            out_specs=(hbm,) * 4,
            scratch_shapes=[dma((4,))],
            compiler_params=pltpu.CompilerParams(vmem_limit_bytes=1024 * 1024),
            name="store",
        )(*results)

    return jax.shard_map(
        shard_step,
        mesh=mesh,
        in_specs=(P("dp"), P("tp", None), P(None), P(None, "tp"), P("tp", None), P(("dp", "tp"), None)),
        out_specs=(P(("dp", "tp"), None), P(("dp", "tp"), None), P("dp", "tp"), P(("dp", "tp"), None)),
        check_vma=False,
    )
```
